32 devices in a mesh: row: 4 (over y, core), col: 8 (over z, x).
Axes of the slice: x: 2, y: 2, z: 4, core: 2. Of those that a mesh axis runs over, the one named last changes fastest.
Arguments:
- amplitudes: float32 [2, 32, 1048576], P(None, 'row', 'col'), may hold values from -6 to 6
- qubit_order: int32 [11], replicated, may hold values from 0 to 10, each once
Outputs:
- correlators: float32 [8, 131072], P('col', 'row')
The draws below stay inside these ranges and needn't reach their ends.
Inputs may be any that keep to these rules, and one draw needn't show every extreme that they name: `qubit_order`: a permutation of 0 to 10.
All inputs are finite; a program needn't handle non-finite values.
Results may differ from the reference program's by a relative error of at most 0.0003.
Values sent between devices are 32-bit elements; how exact they have to be, the bound alone decides.
No kernel may reach another device: no remote copies, remote signals or barrier semaphores. Data moves between devices by JAX's collectives and lax.ppermute only.
A program may use at most 64 MiB of HBM per device.

```python
import jax
import jax.numpy as jnp

MEASURED_QUBITS = 20
PERM_BITS = 11
UNMEASURED = 32
OUTCOMES = 1048576
SLICE = 131072


def shard_levels(key, dims, cuts, low, top_value):
    level, own = 1.0, jax.random.fold_in(key, 6)
    for position, blocks in cuts:
        heights = jnp.exp(jax.random.uniform(jax.random.fold_in(own, position), (blocks,), jnp.float32, low / len(cuts), top_value / len(cuts)))
        level = level * jnp.repeat(heights, dims[position] // blocks).reshape([-1 if axis == position else 1 for axis in range(len(dims))])
    return level


def bell_draw(own_key, extent, scale, reach, cuts=(), held_as=jnp.bfloat16):
    drawn = jax.random.normal(own_key, extent, jnp.float32) * scale
    if len(cuts) > 0:
        drawn = shard_levels(own_key, extent, cuts, -0.22, 0.18) * drawn
    return jnp.clip(drawn, min=-reach, max=reach).astype(held_as)


def setup_inputs(seed: int = 0) -> dict:
    key_list = jax.random.split(jax.random.key(seed), 3)
    amplitudes = bell_draw(key_list[0], (2, UNMEASURED, OUTCOMES), 1.0, 6.0, ((1, 4), (2, 8)), jnp.float32)
    qubit_order = jax.random.permutation(key_list[1], PERM_BITS).astype(jnp.int32)
    return {"amplitudes": amplitudes, "qubit_order": qubit_order}


def source_index(qubit_order):
    count = qubit_order.shape[0]
    target = jnp.arange(2 ** count, dtype=jnp.int32)
    source = jnp.zeros_like(target)
    for bit_location in range(count):
        bit_value = jnp.bitwise_and(jnp.right_shift(target, bit_location), 1)
        source = source + jnp.left_shift(bit_value, qubit_order[bit_location].astype(jnp.int32))
    return source.astype(jnp.int32)


def reference(amplitudes, qubit_order):
    marginal = jnp.sum(amplitudes * amplitudes, axis=(0, 1))
    probability_total = jnp.sum(marginal)
    perm_span = 2 ** qubit_order.shape[0]
    ordered = jnp.take(marginal.reshape(-1, perm_span), source_index(qubit_order), axis=1).reshape(-1)
    walsh_coefficients = ordered
    for bit_location in range(MEASURED_QUBITS):
        folded = walsh_coefficients.reshape(-1, 2, 2 ** bit_location)
        walsh_coefficients = jnp.stack([folded[:, 0] + folded[:, 1], folded[:, 0] - folded[:, 1]], axis=1).reshape(-1)
    correlators = walsh_coefficients * (2.0 ** (MEASURED_QUBITS / 2)) / probability_total
    return correlators.reshape(OUTCOMES // SLICE, SLICE)
```

```python
import jax
import jax.numpy as jnp
from jax import lax
from jax.experimental import pallas as pl
from jax.experimental.pallas import tpu as pltpu
from jax.sharding import PartitionSpec as P

LANES = 128
SUB = 8
ROW_SIDE = 16
CHUNK = ROW_SIDE * ROW_SIDE * LANES


def log2(n):
    return n.bit_length() - 1


def parity_sign(common, bits):
    shift = 1
    while shift < bits:
        common = jnp.bitwise_xor(common, jnp.right_shift(common, shift))
        shift *= 2
    return (1 - 2 * jnp.bitwise_and(common, 1)).astype(jnp.float32)


def iota(shape, axis):
    return lax.broadcasted_iota(jnp.int32, shape, axis)


def bit_of(values, position):
    return jnp.bitwise_and(jnp.right_shift(values, position), 1)


def split(values):
    high = values.astype(jnp.bfloat16)
    low = (values - high.astype(jnp.float32)).astype(jnp.bfloat16)
    return jnp.concatenate([high, low], axis=1)


def transform_kernel(order, amps, out, mass, buf, xs, hrow, hlane, inverse, rows_moved, lanes_moved, sems):
    parts, groups, length = buf.shape[0], buf.shape[1] // SUB, buf.shape[2]
    chunks = length // CHUNK
    half = CHUNK // 2
    lane_bits, row_bits = log2(LANES), log2(ROW_SIDE)
    count = order.shape[0]

    def copies(c):
        return [
            pltpu.make_async_copy(
                amps.at[p, :, pl.ds(c * CHUNK + h * half, half)],
                buf.at[p, :, pl.ds(c * CHUNK + h * half, half)],
                sems.at[c, p, h],
            )
            for p in range(parts)
            for h in range(2)
        ]

    for c in range(min(2, chunks)):
        for copy in copies(c):
            copy.start()

    for j in range(count):
        inverse[order[j]] = j
    for p in range(count + 1):
        rows_moved[p] = lane_bits
        lanes_moved[p] = 0
    moved = jnp.int32(0)
    for p in range(lane_bits, count):
        rows_moved[moved] = p
        moved = moved + (inverse[p] < lane_bits).astype(jnp.int32)
    moved = jnp.int32(0)
    for p in range(lane_bits):
        lanes_moved[moved] = p
        moved = moved + (inverse[p] >= lane_bits).astype(jnp.int32)

    lane = iota((1, LANES), 1)
    zero = jnp.zeros((1, LANES), jnp.int32)
    lane_index, row_flip, lane_from_row = zero, zero, [jnp.int32(0)] * row_bits
    rank = jnp.int32(0)
    for p in range(lane_bits):
        crosses = inverse[p] >= lane_bits
        partner = rows_moved[rank]
        source = jnp.where(crosses, inverse[jnp.where(crosses, partner, 0)], inverse[p])
        lane_index = lane_index + jnp.left_shift(bit_of(lane, source), p)
        row_flip = row_flip + jnp.where(crosses, jnp.left_shift(bit_of(lane, p), partner - lane_bits), 0)
        for r in range(row_bits):
            lane_from_row[r] = lane_from_row[r] + jnp.where(
                jnp.logical_and(crosses, partner == lane_bits + r), jnp.int32(1 << p), jnp.int32(0)
            )
        rank = rank + crosses.astype(jnp.int32)

    out_row_flip, row_target = zero, []
    rank = jnp.int32(0)
    for p in range(lane_bits, count):
        crosses = inverse[p] < lane_bits
        out_row_flip = out_row_flip + jnp.where(
            crosses, jnp.left_shift(bit_of(lane, jnp.where(crosses, inverse[p], 0)), p - lane_bits), 0
        )
        partner = lanes_moved[rank]
        row_target.append(jnp.where(crosses, inverse[jnp.where(crosses, partner, 0)], inverse[p]) - lane_bits)
        rank = rank + crosses.astype(jnp.int32)

    side = ROW_SIDE * ROW_SIDE
    column = iota((1, side), 1)
    low = jnp.right_shift(column, row_bits)
    low_target = jnp.zeros((1, side), jnp.int32)
    for p in range(row_bits):
        low_target = low_target + jnp.left_shift(bit_of(low, p), row_target[p])
    source = jnp.left_shift(jnp.bitwise_and(column, ROW_SIDE - 1), row_bits) + low_target
    hrow[...] = parity_sign(jnp.bitwise_and(iota((side, side), 0), source), 2 * row_bits).astype(jnp.bfloat16)
    stacked = (2 * LANES, LANES)
    lane_sign = parity_sign(
        jnp.bitwise_and(jnp.bitwise_and(iota(stacked, 0), LANES - 1), iota(stacked, 1)), lane_bits
    )
    hlane[...] = lane_sign.astype(jnp.bfloat16)

    flips = [bit_of(row_flip, r) == 1 for r in range(row_bits)]
    out_flips = [bit_of(out_row_flip, r) == 1 for r in range(row_bits)]
    gathers = []
    for i in range(ROW_SIDE):
        moved = jnp.int32(0)
        for r in range(row_bits):
            if i >> r & 1:
                moved = moved + lane_from_row[r]
        gathers.append(jnp.broadcast_to(jnp.bitwise_xor(lane_index, moved), (ROW_SIDE, LANES)))

    sub = iota((SUB, LANES), 0)
    masks = [bit_of(sub, level) == 0 for level in range(log2(SUB))]

    def packed_row(base, i, upper):
        tiles = []
        for s in range(SUB):
            start = base + ((upper * SUB + s) * ROW_SIDE + i) * LANES
            total = None
            for p in range(parts):
                for g in range(groups):
                    v = buf[p, g * SUB : (g + 1) * SUB, pl.ds(start, LANES)]
                    total = v * v if total is None else total + v * v
            tiles.append(total)
        for level in range(log2(SUB)):
            merged = []
            for k in range(0, len(tiles), 2):
                a, b = tiles[k], tiles[k + 1]
                kept = jnp.where(masks[level], a, b)
                other = jnp.where(masks[level], b, a)
                merged.append(kept + pltpu.roll(other, SUB - (1 << level), 0))
            tiles = merged
        return tiles[0]

    def flip_rows(rows, which):
        for r in range(row_bits):
            rows = [jnp.where(which[r], rows[i ^ 1 << r], rows[i]) for i in range(ROW_SIDE)]
        return rows

    def one_chunk(c, total):
        for copy in copies(c):
            copy.wait()

        @pl.when(c + 2 < chunks)
        def _():
            for copy in copies(c + 2):
                copy.start()

        base = pl.multiple_of(c * CHUNK, CHUNK)
        for i in range(ROW_SIDE):
            for upper in range(ROW_SIDE // SUB):
                packed = packed_row(base, i, upper)
                total = total + packed
                xs[i, upper * SUB : (upper + 1) * SUB, :] = packed
        rows = flip_rows([xs[i] for i in range(ROW_SIDE)], flips)
        rows = [jnp.take_along_axis(rows[i], gathers[i], axis=1) for i in range(ROW_SIDE)]
        rows = flip_rows(rows, out_flips)
        x = split(jnp.concatenate(rows, axis=0))
        y = jnp.dot(hrow[...], x, preferred_element_type=jnp.float32)
        y = split(y[:, :LANES] + y[:, LANES:])
        z = jnp.dot(y, hlane[...], preferred_element_type=jnp.float32)
        out[pl.ds(pl.multiple_of(c * side, side), side), :] = z
        return total

    mass[...] = lax.fori_loop(0, chunks, one_chunk, jnp.zeros((SUB, LANES), jnp.float32))

    stride = 1
    while stride < chunks:
        for c in range(chunks):
            if c & stride == 0:
                a_rows, b_rows = pl.ds(c * side, side), pl.ds((c + stride) * side, side)
                a, b = out[a_rows, :], out[b_rows, :]
                out[a_rows, :] = a + b
                out[b_rows, :] = a - b
        stride *= 2


def transform_local(amplitudes, qubit_order):
    parts, unmeasured, length = amplitudes.shape
    chunks = length // CHUNK
    side = ROW_SIDE * ROW_SIDE
    count = qubit_order.shape[0]
    return pl.pallas_call(
        transform_kernel,
        out_shape=(
            jax.ShapeDtypeStruct((chunks * side, LANES), jnp.float32),
            jax.ShapeDtypeStruct((SUB, LANES), jnp.float32),
        ),
        in_specs=[pl.BlockSpec(memory_space=pltpu.SMEM), pl.BlockSpec(memory_space=pl.ANY)],
        out_specs=(pl.BlockSpec(memory_space=pltpu.VMEM), pl.BlockSpec(memory_space=pltpu.VMEM)),
        scratch_shapes=[
            pltpu.VMEM((parts, unmeasured, length), jnp.float32),
            pltpu.VMEM((ROW_SIDE, ROW_SIDE, LANES), jnp.float32),
            pltpu.VMEM((side, side), jnp.bfloat16),
            pltpu.VMEM((2 * LANES, LANES), jnp.bfloat16),
            pltpu.SMEM((count,), jnp.int32),
            pltpu.SMEM((count + 1,), jnp.int32),
            pltpu.SMEM((count + 1,), jnp.int32),
            pltpu.SemaphoreType.DMA((chunks, parts, 2)),
        ],
        name="transform_local",
    )(qubit_order, amplitudes)


def exchange(message, axis, position):
    size = lax.axis_size(axis)
    return lax.ppermute(message, axis, [(i, i ^ 1 << position) for i in range(size)])


def local(amplitudes, qubit_order, measured_qubits):
    values, mass = transform_local(amplitudes, qubit_order)
    blocks = lax.axis_size("row")
    share = values.shape[0] // blocks
    for position in range(log2(blocks)):
        pairs = values.reshape(-1, 2, share, LANES)
        high = bit_of(lax.axis_index("row"), position) == 1
        kept = jnp.where(high, pairs[:, 1], pairs[:, 0]).reshape(-1, LANES)
        sent = jnp.where(high, pairs[:, 0], pairs[:, 1]).reshape(-1, LANES)
        received = exchange(jnp.concatenate([sent, mass]), "row", position)
        joined = jnp.concatenate([kept, mass]) + received
        values, mass = joined[:-SUB], joined[-SUB:]
    joined = jnp.concatenate([values, mass])
    plain = iota((joined.shape[0], 1), 0) >= share
    for position in range(log2(lax.axis_size("col"))):
        received = exchange(joined, "col", position)
        low = bit_of(lax.axis_index("col"), position) == 0
        joined = received + jnp.where(jnp.logical_or(plain, low), joined, -joined)
    total = jnp.sum(joined[-SUB:])
    return (joined[:-SUB] * 2.0 ** (measured_qubits / 2) / total).reshape(1, -1)


def solution(mesh):
    def program(amplitudes, qubit_order):
        measured_qubits = log2(amplitudes.shape[2])
        return jax.shard_map(
            lambda a, q: local(a, q, measured_qubits),
            mesh=mesh,
            in_specs=(P(None, "row", "col"), P()),
            out_specs=P("col", "row"),
            check_vma=False,
        )(amplitudes, qubit_order)

    return program
```

```python
import functools

import jax
import jax.numpy as jnp
from jax import lax
from jax.experimental import pallas as pl
from jax.experimental.pallas import tpu as pltpu
from jax.sharding import PartitionSpec as P

LANES = 128
SUB = 8
ROW_SIDE = 16
CHUNK = ROW_SIDE * ROW_SIDE * LANES


def log2(n):
    return n.bit_length() - 1


def parity_sign(common, bits):
    shift = 1
    while shift < bits:
        common = jnp.bitwise_xor(common, jnp.right_shift(common, shift))
        shift *= 2
    return (1 - 2 * jnp.bitwise_and(common, 1)).astype(jnp.float32)


def iota(shape, axis):
    return lax.broadcasted_iota(jnp.int32, shape, axis)


def bit_of(values, position):
    return jnp.bitwise_and(jnp.right_shift(values, position), 1)


def split(values):
    high = values.astype(jnp.bfloat16)
    low = (values - high.astype(jnp.float32)).astype(jnp.bfloat16)
    return jnp.concatenate([high, low], axis=1)


def transform_kernel(row_axis, order, amps, sent, kept, buf, out, xs, hrow, hlane, inverse, rows_moved, lanes_moved, sems):
    parts, groups, length = buf.shape[0], buf.shape[1] // SUB, buf.shape[2]
    chunks = length // CHUNK
    half = CHUNK // 2
    lane_bits, row_bits = log2(LANES), log2(ROW_SIDE)
    count = order.shape[0]

    def copies(c):
        return [
            pltpu.make_async_copy(
                amps.at[p, :, pl.ds(c * CHUNK + h * half, half)],
                buf.at[p, :, pl.ds(c * CHUNK + h * half, half)],
                sems.at[c, p, h],
            )
            for p in range(parts)
            for h in range(2)
        ]

    for c in range(min(2, chunks)):
        for copy in copies(c):
            copy.start()

    for j in range(count):
        inverse[order[j]] = j
    for p in range(count + 1):
        rows_moved[p] = lane_bits
        lanes_moved[p] = 0
    moved = jnp.int32(0)
    for p in range(lane_bits, count):
        rows_moved[moved] = p
        moved = moved + (inverse[p] < lane_bits).astype(jnp.int32)
    moved = jnp.int32(0)
    for p in range(lane_bits):
        lanes_moved[moved] = p
        moved = moved + (inverse[p] >= lane_bits).astype(jnp.int32)

    lane = iota((1, LANES), 1)
    zero = jnp.zeros((1, LANES), jnp.int32)
    lane_index, row_flip, lane_from_row = zero, zero, [jnp.int32(0)] * row_bits
    rank = jnp.int32(0)
    for p in range(lane_bits):
        crosses = inverse[p] >= lane_bits
        partner = rows_moved[rank]
        source = jnp.where(crosses, inverse[jnp.where(crosses, partner, 0)], inverse[p])
        lane_index = lane_index + jnp.left_shift(bit_of(lane, source), p)
        row_flip = row_flip + jnp.where(crosses, jnp.left_shift(bit_of(lane, p), partner - lane_bits), 0)
        for r in range(row_bits):
            lane_from_row[r] = lane_from_row[r] + jnp.where(
                jnp.logical_and(crosses, partner == lane_bits + r), jnp.int32(1 << p), jnp.int32(0)
            )
        rank = rank + crosses.astype(jnp.int32)

    out_row_flip, row_target = zero, []
    rank = jnp.int32(0)
    for p in range(lane_bits, count):
        crosses = inverse[p] < lane_bits
        out_row_flip = out_row_flip + jnp.where(
            crosses, jnp.left_shift(bit_of(lane, jnp.where(crosses, inverse[p], 0)), p - lane_bits), 0
        )
        partner = lanes_moved[rank]
        row_target.append(jnp.where(crosses, inverse[jnp.where(crosses, partner, 0)], inverse[p]) - lane_bits)
        rank = rank + crosses.astype(jnp.int32)

    side = ROW_SIDE * ROW_SIDE
    column = iota((1, side), 1)
    low = jnp.right_shift(column, row_bits)
    low_target = jnp.zeros((1, side), jnp.int32)
    for p in range(row_bits):
        low_target = low_target + jnp.left_shift(bit_of(low, p), row_target[p])
    source = jnp.left_shift(jnp.bitwise_and(column, ROW_SIDE - 1), row_bits) + low_target
    hrow[...] = parity_sign(jnp.bitwise_and(iota((side, side), 0), source), 2 * row_bits).astype(jnp.bfloat16)
    stacked = (2 * LANES, LANES)
    lane_sign = parity_sign(
        jnp.bitwise_and(jnp.bitwise_and(iota(stacked, 0), LANES - 1), iota(stacked, 1)), lane_bits
    )
    hlane[...] = lane_sign.astype(jnp.bfloat16)

    flips = [bit_of(row_flip, r) == 1 for r in range(row_bits)]
    out_flips = [bit_of(out_row_flip, r) == 1 for r in range(row_bits)]
    gathers = []
    for i in range(ROW_SIDE):
        moved = jnp.int32(0)
        for r in range(row_bits):
            if i >> r & 1:
                moved = moved + lane_from_row[r]
        gathers.append(jnp.broadcast_to(jnp.bitwise_xor(lane_index, moved), (ROW_SIDE, LANES)))

    sub = iota((SUB, LANES), 0)
    masks = [bit_of(sub, level) == 0 for level in range(log2(SUB))]

    def packed_row(base, i, upper):
        tiles = []
        for s in range(SUB):
            start = base + ((upper * SUB + s) * ROW_SIDE + i) * LANES
            total = None
            for p in range(parts):
                for g in range(groups):
                    v = buf[p, g * SUB : (g + 1) * SUB, pl.ds(start, LANES)]
                    total = v * v if total is None else total + v * v
            tiles.append(total)
        for level in range(log2(SUB)):
            merged = []
            for k in range(0, len(tiles), 2):
                a, b = tiles[k], tiles[k + 1]
                kept = jnp.where(masks[level], a, b)
                other = jnp.where(masks[level], b, a)
                merged.append(kept + pltpu.roll(other, SUB - (1 << level), 0))
            tiles = merged
        return tiles[0]

    def flip_rows(rows, which):
        for r in range(row_bits):
            rows = [jnp.where(which[r], rows[i ^ 1 << r], rows[i]) for i in range(ROW_SIDE)]
        return rows

    def one_chunk(c, total):
        for copy in copies(c):
            copy.wait()

        @pl.when(c + 2 < chunks)
        def _():
            for copy in copies(c + 2):
                copy.start()

        base = pl.multiple_of(c * CHUNK, CHUNK)
        for i in range(ROW_SIDE):
            for upper in range(ROW_SIDE // SUB):
                packed = packed_row(base, i, upper)
                total = total + packed
                xs[i, upper * SUB : (upper + 1) * SUB, :] = packed
        rows = flip_rows([xs[i] for i in range(ROW_SIDE)], flips)
        rows = [jnp.take_along_axis(rows[i], gathers[i], axis=1) for i in range(ROW_SIDE)]
        rows = flip_rows(rows, out_flips)
        x = split(jnp.concatenate(rows, axis=0))
        y = jnp.dot(hrow[...], x, preferred_element_type=jnp.float32)
        y = split(y[:, :LANES] + y[:, LANES:])
        z = jnp.dot(y, hlane[...], preferred_element_type=jnp.float32)
        out[pl.ds(pl.multiple_of(c * side, side), side), :] = z
        return total

    total = lax.fori_loop(0, chunks, one_chunk, jnp.zeros((SUB, LANES), jnp.float32))
    total = jnp.broadcast_to(jnp.sum(total, keepdims=True), (SUB, LANES))

    stride = 1
    while stride < chunks:
        for c in range(chunks):
            if c & stride == 0:
                a_rows, b_rows = pl.ds(c * side, side), pl.ds((c + stride) * side, side)
                a, b = out[a_rows, :], out[b_rows, :]
                out[a_rows, :] = a + b
                out[b_rows, :] = a - b
        stride *= 2

    blocks = lax.axis_size(row_axis)
    share = out.shape[0] // blocks
    own_bit = bit_of(lax.axis_index(row_axis), 0)
    for ref, bit in ((sent, 1 - own_bit), (kept, own_bit)):
        for pair in range(blocks // 2):
            start = pl.multiple_of((2 * pair + bit) * share, share)
            ref[pair * share : (pair + 1) * share, :] = out[pl.ds(start, share), :]
        ref[blocks // 2 * share :, :] = total


def transform_local(amplitudes, qubit_order, row_axis):
    parts, unmeasured, length = amplitudes.shape
    chunks = length // CHUNK
    side = ROW_SIDE * ROW_SIDE
    count = qubit_order.shape[0]
    message = pltpu.VMEM((chunks * side // 2 + SUB, LANES), jnp.float32)
    return pl.pallas_call(
        functools.partial(transform_kernel, row_axis),
        out_shape=(message, message),
        in_specs=[pl.BlockSpec(memory_space=pltpu.SMEM), pl.BlockSpec(memory_space=pl.ANY)],
        out_specs=(pl.BlockSpec(memory_space=pltpu.VMEM), pl.BlockSpec(memory_space=pltpu.VMEM)),
        scratch_shapes=[
            pltpu.VMEM((parts, unmeasured, length), jnp.float32),
            pltpu.VMEM((chunks * side, LANES), jnp.float32),
            pltpu.VMEM((ROW_SIDE, ROW_SIDE, LANES), jnp.float32),
            pltpu.VMEM((side, side), jnp.bfloat16),
            pltpu.VMEM((2 * LANES, LANES), jnp.bfloat16),
            pltpu.SMEM((count,), jnp.int32),
            pltpu.SMEM((count + 1,), jnp.int32),
            pltpu.SMEM((count + 1,), jnp.int32),
            pltpu.SemaphoreType.DMA((chunks, parts, 2)),
        ],
        name="transform_local",
    )(qubit_order, amplitudes)


def exchange(message, axis, position):
    size = lax.axis_size(axis)
    return lax.ppermute(message, axis, [(i, i ^ 1 << position) for i in range(size)])


def local(amplitudes, qubit_order, measured_qubits):
    sent, kept = transform_local(amplitudes, qubit_order, "row")
    joined = kept + exchange(sent, "row", 0)
    row_bits = log2(lax.axis_size("row"))
    share = (joined.shape[0] - SUB) >> row_bits - 1
    for position in range(1, row_bits):
        pairs = joined[:-SUB].reshape(-1, 2, share, LANES)
        mass = joined[-SUB:]
        high = bit_of(lax.axis_index("row"), position) == 1
        kept = jnp.where(high, pairs[:, 1], pairs[:, 0]).reshape(-1, LANES)
        sent = jnp.where(high, pairs[:, 0], pairs[:, 1]).reshape(-1, LANES)
        joined = jnp.concatenate([kept, mass]) + exchange(jnp.concatenate([sent, mass]), "row", position)
    values, mass = joined[:-SUB], joined[-SUB:]
    for position in range(log2(lax.axis_size("col"))):
        received = exchange(jnp.concatenate([values, mass]), "col", position)
        sign = 1.0 - 2.0 * bit_of(lax.axis_index("col"), position).astype(jnp.float32)
        values = received[:-SUB] + values * sign
        mass = received[-SUB:] + mass
    total = mass[:1]
    return (values * 2.0 ** (measured_qubits / 2) / total).reshape(1, -1)


def solution(mesh):
    def program(amplitudes, qubit_order):
        measured_qubits = log2(amplitudes.shape[2])
        return jax.shard_map(
            lambda a, q: local(a, q, measured_qubits),
            mesh=mesh,
            in_specs=(P(None, "row", "col"), P()),
            out_specs=P("col", "row"),
            check_vma=False,
        )(amplitudes, qubit_order)

    return program
```

```python
import functools

import jax
import jax.numpy as jnp
from jax import lax
from jax.experimental import pallas as pl
from jax.experimental.pallas import tpu as pltpu
from jax.sharding import PartitionSpec as P

LANES = 128
SUB = 8
ROW_SIDE = 16
CHUNK = ROW_SIDE * ROW_SIDE * LANES


def log2(n):
    return n.bit_length() - 1


def parity_sign(common, bits):
    shift = 1
    while shift < bits:
        common = jnp.bitwise_xor(common, jnp.right_shift(common, shift))
        shift *= 2
    return (1 - 2 * jnp.bitwise_and(common, 1)).astype(jnp.float32)


def iota(shape, axis):
    return lax.broadcasted_iota(jnp.int32, shape, axis)


def bit_of(values, position):
    return jnp.bitwise_and(jnp.right_shift(values, position), 1)


def split(values):
    high = values.astype(jnp.bfloat16)
    low = (values - high.astype(jnp.float32)).astype(jnp.bfloat16)
    return jnp.concatenate([high, low], axis=1)


def transform_kernel(
    row_axis, order_in, amps, messages, buf, out, xs, hlane,
    order, inverse, rows_moved, lanes_moved, row_target, row_unit, lane_unit, order_sem, sems,
):
    parts, groups, length = buf.shape[0], buf.shape[1] // SUB, buf.shape[2]
    chunks = length // CHUNK
    half = CHUNK // 2
    side = ROW_SIDE * ROW_SIDE
    lane_bits, row_bits = log2(LANES), log2(ROW_SIDE)
    count = order.shape[0]

    def copies(step):
        return [
            pltpu.make_async_copy(
                amps.at[p, :, pl.ds(step * half, half)], buf.at[p, :, pl.ds(step * half, half)], sems.at[step, p]
            )
            for p in range(parts)
        ]

    order_copy = pltpu.make_async_copy(order_in, order, order_sem)
    order_copy.start()
    for step in range(2 * chunks):
        for copy in copies(step):
            copy.start()

    stacked = (2 * LANES, LANES)
    lane_sign = parity_sign(
        jnp.bitwise_and(jnp.bitwise_and(iota(stacked, 0), LANES - 1), iota(stacked, 1)), lane_bits
    )
    hlane[...] = lane_sign.astype(jnp.bfloat16)
    for p in range(count + 1):
        rows_moved[p] = lane_bits
        lanes_moved[p] = 0
    for r in range(row_bits + 1):
        lane_unit[r] = 0
    order_copy.wait()

    for j in range(count):
        inverse[order[j]] = j
    rank = jnp.int32(0)
    for p in range(lane_bits):
        lanes_moved[rank] = p
        rank = rank + (inverse[p] >= lane_bits).astype(jnp.int32)
    lane = iota((1, LANES), 1)
    lane_index = row_flip = out_row_flip = jnp.zeros((1, LANES), jnp.int32)
    rank = jnp.int32(0)
    for p in range(lane_bits, count):
        goes_to = inverse[p]
        crosses = goes_to < lane_bits
        rows_moved[rank] = p
        target = inverse[jnp.where(crosses, lanes_moved[rank], p)] - lane_bits
        row_target[p - lane_bits] = target
        row_unit[target] = 1 << p - lane_bits
        flip = jnp.left_shift(bit_of(lane, jnp.where(crosses, goes_to, 0)), target)
        out_row_flip = out_row_flip + jnp.where(crosses, flip, 0)
        rank = rank + crosses.astype(jnp.int32)
    rank = jnp.int32(0)
    for p in range(lane_bits):
        crosses = inverse[p] >= lane_bits
        partner = rows_moved[rank]
        lane_index = lane_index + jnp.left_shift(bit_of(lane, inverse[jnp.where(crosses, partner, p)]), p)
        target = row_target[jnp.where(crosses, partner - lane_bits, 0)]
        row_flip = row_flip + jnp.where(crosses, jnp.left_shift(bit_of(lane, p), target), 0)
        lane_unit[jnp.where(crosses, target, row_bits)] = 1 << p
        rank = rank + crosses.astype(jnp.int32)

    flips = [bit_of(row_flip, r) == 1 for r in range(row_bits)]
    out_flips = [bit_of(out_row_flip, r) == 1 for r in range(row_bits)]
    sources, gathers = [jnp.int32(0)], [jnp.int32(0)]
    for r in range(row_bits):
        sources = sources + [source + row_unit[r] for source in sources]
        gathers = gathers + [gather + lane_unit[r] for gather in gathers]
    gathers = [jnp.broadcast_to(jnp.bitwise_xor(lane_index, gather), (ROW_SIDE, LANES)) for gather in gathers]

    sub = iota((SUB, LANES), 0)
    masks = [bit_of(sub, level) == 0 for level in range(log2(SUB))]

    def packed_row(base, i):
        tiles = []
        for s in range(SUB):
            start = base + (s * ROW_SIDE + i) * LANES
            total = None
            for p in range(parts):
                for g in range(groups):
                    v = buf[p, g * SUB : (g + 1) * SUB, pl.ds(start, LANES)]
                    total = v * v if total is None else total + v * v
            tiles.append(total)
        for level in range(log2(SUB)):
            merged = []
            for k in range(0, len(tiles), 2):
                a, b = tiles[k] + tiles[k + 1], tiles[k] - tiles[k + 1]
                here = jnp.where(masks[level], a, b)
                other = jnp.where(masks[level], b, a)
                merged.append(here + pltpu.roll(other, SUB - (1 << level), 0))
            tiles = merged
        return tiles[0]

    def flip_rows(rows, which):
        for r in range(row_bits):
            rows = [jnp.where(which[r], rows[i ^ 1 << r], rows[i]) for i in range(ROW_SIDE)]
        return rows

    def butterfly(blocks, stride):
        return [
            blocks[c ^ stride] - blocks[c] if c & stride else blocks[c] + blocks[c ^ stride] for c in range(len(blocks))
        ]

    def arrive(step):
        for copy in copies(step):
            copy.wait()

    def sums(step, upper, total):
        base = pl.multiple_of(step * half, half)
        for i in range(ROW_SIDE):
            packed = packed_row(base, i)
            total = total + packed
            xs[i, upper * SUB : (upper + 1) * SUB, :] = packed
        return total

    def transform(c):
        rows = flip_rows([xs[source] for source in sources], flips)
        rows = [jnp.take_along_axis(rows[i], gathers[i], axis=1) for i in range(ROW_SIDE)]
        rows = flip_rows(rows, out_flips)
        for r in range(row_bits):
            rows = butterfly(rows, 1 << r)
        rows = [
            jnp.concatenate(butterfly([row[upper * SUB : (upper + 1) * SUB] for upper in range(2)], 1), axis=0)
            for row in rows
        ]
        z = jnp.dot(split(jnp.concatenate(rows, axis=0)), hlane[...], preferred_element_type=jnp.float32)
        first = pl.multiple_of(c * side, side)
        for i in range(ROW_SIDE):
            out[pl.ds(first + i, ROW_SIDE, stride=ROW_SIDE), :] = z[i * ROW_SIDE : (i + 1) * ROW_SIDE]

    def one_chunk(c, total):
        arrive(2 * c)
        transform(c - 1)
        total = sums(2 * c, 0, total)
        arrive(2 * c + 1)
        return sums(2 * c + 1, 1, total)

    total = jnp.zeros((SUB, LANES), jnp.float32)
    for upper in range(2):
        arrive(upper)
        total = sums(upper, upper, total)
    total = lax.fori_loop(1, chunks, one_chunk, total)
    transform(chunks - 1)
    total = jnp.broadcast_to(jnp.sum(total[:1], keepdims=True), (SUB, LANES))

    blocks = lax.axis_size(row_axis)
    share = out.shape[0] // blocks
    own_bit = bit_of(lax.axis_index(row_axis), 0)
    kept = messages.shape[0] // 2
    strides = [1 << k for k in range(log2(chunks))]
    apart = share // side
    rows = min(side, 4 * SUB)
    own_sign = 1.0 - 2.0 * own_bit.astype(jnp.float32)
    for start in range(0, side, rows):
        blocks_in = [out[c * side + start : c * side + start + rows, :] for c in range(chunks)]
        for stride in strides:
            if stride != apart:
                blocks_in = butterfly(blocks_in, stride)
        for c in range(chunks):
            if apart == 0:
                out[c * side + start : c * side + start + rows, :] = blocks_in[c]
            elif c & apart == 0:
                low, high = blocks_in[c], own_sign * blocks_in[c ^ apart]
                at = (c // (2 * apart) * apart + c % apart) * side + start
                messages[at : at + rows, :] = low - high
                messages[kept + at : kept + at + rows, :] = low + high
    if apart == 0:
        for at, bit in ((0, 1 - own_bit), (kept, own_bit)):
            for pair in range(blocks // 2):
                start = pl.multiple_of((2 * pair + bit) * share, share)
                messages[at + pair * share : at + (pair + 1) * share, :] = out[pl.ds(start, share), :]
    for at in (0, kept):
        messages[at + kept - SUB : at + kept, :] = total


def transform_local(amplitudes, qubit_order, row_axis):
    parts, unmeasured, length = amplitudes.shape
    chunks = length // CHUNK
    side = ROW_SIDE * ROW_SIDE
    count = qubit_order.shape[0]
    return pl.pallas_call(
        functools.partial(transform_kernel, row_axis),
        out_shape=pltpu.VMEM((chunks * side + 2 * SUB, LANES), jnp.float32),
        in_specs=[pl.BlockSpec(memory_space=pl.ANY), pl.BlockSpec(memory_space=pl.ANY)],
        out_specs=pl.BlockSpec(memory_space=pltpu.VMEM),
        scratch_shapes=[
            pltpu.VMEM((parts, unmeasured, length), jnp.float32),
            pltpu.VMEM((chunks * side, LANES), jnp.float32),
            pltpu.VMEM((ROW_SIDE, ROW_SIDE, LANES), jnp.float32),
            pltpu.VMEM((2 * LANES, LANES), jnp.bfloat16),
            pltpu.SMEM((count,), jnp.int32),
            *[pltpu.SMEM((count + 1,), jnp.int32) for _ in range(6)],
            pltpu.SemaphoreType.DMA(()),
            pltpu.SemaphoreType.DMA((2 * chunks, parts)),
        ],
        name="transform_local",
    )(qubit_order, amplitudes)


def exchange(message, axis, position):
    size = lax.axis_size(axis)
    return lax.ppermute(message, axis, [(i, i ^ 1 << position) for i in range(size)])


def local(amplitudes, qubit_order, measured_qubits):
    messages = transform_local(amplitudes, qubit_order, "row")
    rows = messages.shape[0] // 2
    joined = messages[rows:] + exchange(messages[:rows], "row", 0)
    row_bits = log2(lax.axis_size("row"))
    share = (joined.shape[0] - SUB) >> row_bits - 1
    for position in range(1, row_bits):
        pairs = joined[:-SUB].reshape(-1, 2, share, LANES)
        mass = joined[-SUB:]
        high = bit_of(lax.axis_index("row"), position) == 1
        kept = jnp.where(high, pairs[:, 1], pairs[:, 0]).reshape(-1, LANES)
        sent = jnp.where(high, pairs[:, 0], pairs[:, 1]).reshape(-1, LANES)
        joined = jnp.concatenate([kept, mass]) + exchange(jnp.concatenate([sent, mass]), "row", position)
    values, mass = joined[:-SUB], joined[-SUB:]
    for position in range(log2(lax.axis_size("col"))):
        received = exchange(jnp.concatenate([values, mass]), "col", position)
        sign = 1.0 - 2.0 * bit_of(lax.axis_index("col"), position).astype(jnp.float32)
        values = received[:-SUB] + values * sign
        mass = received[-SUB:] + mass
    total = mass[:1]
    return (values * 2.0 ** (measured_qubits / 2) / total).reshape(1, -1)


def solution(mesh):
    def program(amplitudes, qubit_order):
        measured_qubits = log2(amplitudes.shape[2])
        return jax.shard_map(
            lambda a, q: local(a, q, measured_qubits),
            mesh=mesh,
            in_specs=(P(None, "row", "col"), P()),
            out_specs=P("col", "row"),
            check_vma=False,
        )(amplitudes, qubit_order)

    return program
```

```python
import functools

import jax
import jax.numpy as jnp
from jax import lax
from jax.experimental import pallas as pl
from jax.experimental.pallas import tpu as pltpu
from jax.sharding import PartitionSpec as P


LANES = 128
SUB = 8
ROW_SIDE = 16
CHUNK = ROW_SIDE * ROW_SIDE * LANES


def log2(n):
    return n.bit_length() - 1


def parity_sign(common, bits):
    shift = 1
    while shift < bits:
        common = jnp.bitwise_xor(common, jnp.right_shift(common, shift))
        shift *= 2
    return (1 - 2 * jnp.bitwise_and(common, 1)).astype(jnp.float32)


def iota(shape, axis):
    return lax.broadcasted_iota(jnp.int32, shape, axis)


def bit_of(values, position):
    return jnp.bitwise_and(jnp.right_shift(values, position), 1)


def split(values):
    high = values.astype(jnp.bfloat16)
    low = (values - high.astype(jnp.float32)).astype(jnp.bfloat16)
    return jnp.concatenate([high, low], axis=1)


def transform_kernel(
    row_axis, order_in, amps, messages, buf, out, xs, hlane,
    order, inverse, rows_moved, lanes_moved, row_target, row_unit, lane_unit, order_sem, sems,
):
    parts, groups, length = buf.shape[0], buf.shape[1] // SUB, buf.shape[2]
    chunks = length // CHUNK
    half = CHUNK // 2
    side = ROW_SIDE * ROW_SIDE
    lane_bits, row_bits = log2(LANES), log2(ROW_SIDE)
    count = order.shape[0]

    def copies(step):
        return [
            pltpu.make_async_copy(
                amps.at[p, :, pl.ds(step * half, half)], buf.at[p, :, pl.ds(step * half, half)], sems.at[step, p]
            )
            for p in range(parts)
        ]

    order_copy = pltpu.make_async_copy(order_in, order, order_sem)
    order_copy.start()
    for step in range(2 * chunks):
        for copy in copies(step):
            copy.start()

    stacked = (2 * LANES, LANES)
    lane_sign = parity_sign(
        jnp.bitwise_and(jnp.bitwise_and(iota(stacked, 0), LANES - 1), iota(stacked, 1)), lane_bits
    )
    hlane[...] = lane_sign.astype(jnp.bfloat16)
    for p in range(count + 1):
        rows_moved[p] = lane_bits
        lanes_moved[p] = 0
    for r in range(row_bits + 1):
        lane_unit[r] = 0
    order_copy.wait()

    for j in range(count):
        inverse[order[j]] = j
    rank = jnp.int32(0)
    for p in range(lane_bits):
        lanes_moved[rank] = p
        rank = rank + (inverse[p] >= lane_bits).astype(jnp.int32)
    lane = iota((1, LANES), 1)
    lane_index = row_flip = out_row_flip = jnp.zeros((1, LANES), jnp.int32)
    rank = jnp.int32(0)
    for p in range(lane_bits, count):
        goes_to = inverse[p]
        crosses = goes_to < lane_bits
        rows_moved[rank] = p
        target = inverse[jnp.where(crosses, lanes_moved[rank], p)] - lane_bits
        row_target[p - lane_bits] = target
        row_unit[target] = 1 << p - lane_bits
        flip = jnp.left_shift(bit_of(lane, jnp.where(crosses, goes_to, 0)), target)
        out_row_flip = out_row_flip + jnp.where(crosses, flip, 0)
        rank = rank + crosses.astype(jnp.int32)
    rank = jnp.int32(0)
    for p in range(lane_bits):
        crosses = inverse[p] >= lane_bits
        partner = rows_moved[rank]
        lane_index = lane_index + jnp.left_shift(bit_of(lane, inverse[jnp.where(crosses, partner, p)]), p)
        target = row_target[jnp.where(crosses, partner - lane_bits, 0)]
        row_flip = row_flip + jnp.where(crosses, jnp.left_shift(bit_of(lane, p), target), 0)
        lane_unit[jnp.where(crosses, target, row_bits)] = 1 << p
        rank = rank + crosses.astype(jnp.int32)

    flips = [bit_of(row_flip, r) == 1 for r in range(row_bits)]
    out_flips = [bit_of(out_row_flip, r) == 1 for r in range(row_bits)]
    sources, gathers = [jnp.int32(0)], [jnp.int32(0)]
    for r in range(row_bits):
        sources = sources + [source + row_unit[r] for source in sources]
        gathers = gathers + [gather + lane_unit[r] for gather in gathers]
    gathers = [jnp.broadcast_to(jnp.bitwise_xor(lane_index, gather), (ROW_SIDE, LANES)) for gather in gathers]

    sub = iota((SUB, LANES), 0)
    masks = [bit_of(sub, level) == 0 for level in range(log2(SUB))]

    def packed_row(base, i):
        tiles = []
        for s in range(SUB):
            start = base + (s * ROW_SIDE + i) * LANES
            total = None
            for p in range(parts):
                for g in range(groups):
                    v = buf[p, g * SUB : (g + 1) * SUB, pl.ds(start, LANES)]
                    total = v * v if total is None else total + v * v
            tiles.append(total)
        for level in range(log2(SUB)):
            merged = []
            for k in range(0, len(tiles), 2):
                a, b = tiles[k] + tiles[k + 1], tiles[k] - tiles[k + 1]
                here = jnp.where(masks[level], a, b)
                other = jnp.where(masks[level], b, a)
                merged.append(here + pltpu.roll(other, SUB - (1 << level), 0))
            tiles = merged
        return tiles[0]

    def flip_rows(rows, which):
        for r in range(row_bits):
            rows = [jnp.where(which[r], rows[i ^ 1 << r], rows[i]) for i in range(ROW_SIDE)]
        return rows

    def butterfly(blocks, stride):
        return [
            blocks[c ^ stride] - blocks[c] if c & stride else blocks[c] + blocks[c ^ stride] for c in range(len(blocks))
        ]

    def arrive(step):
        for copy in copies(step):
            copy.wait()

    def sums(step, upper, total):
        base = pl.multiple_of(step * half, half)
        for i in range(ROW_SIDE):
            packed = packed_row(base, i)
            total = total + packed
            xs[i, upper * SUB : (upper + 1) * SUB, :] = packed
        return total

    def transform(c):
        rows = flip_rows([xs[source] for source in sources], flips)
        rows = [jnp.take_along_axis(rows[i], gathers[i], axis=1) for i in range(ROW_SIDE)]
        rows = flip_rows(rows, out_flips)
        for r in range(row_bits):
            rows = butterfly(rows, 1 << r)
        rows = [
            jnp.concatenate(butterfly([row[upper * SUB : (upper + 1) * SUB] for upper in range(2)], 1), axis=0)
            for row in rows
        ]
        z = jnp.dot(split(jnp.concatenate(rows, axis=0)), hlane[...], preferred_element_type=jnp.float32)
        first = pl.multiple_of(c * side, side)
        for i in range(ROW_SIDE):
            out[pl.ds(first + i, ROW_SIDE, stride=ROW_SIDE), :] = z[i * ROW_SIDE : (i + 1) * ROW_SIDE]

    def one_chunk(c, total):
        arrive(2 * c)
        transform(c - 1)
        total = sums(2 * c, 0, total)
        arrive(2 * c + 1)
        return sums(2 * c + 1, 1, total)

    total = jnp.zeros((SUB, LANES), jnp.float32)
    for upper in range(2):
        arrive(upper)
        total = sums(upper, upper, total)
    total = lax.fori_loop(1, chunks, one_chunk, total)
    transform(chunks - 1)
    total = jnp.broadcast_to(jnp.sum(total[:1], keepdims=True), (SUB, LANES))

    blocks = lax.axis_size(row_axis)
    share = out.shape[0] // blocks
    own = lax.axis_index(row_axis)
    strides = [1 << k for k in range(log2(chunks))]
    order_of_blocks = [0]
    for k in reversed(range(log2(blocks))):
        order_of_blocks = order_of_blocks + [j + (1 << k) for j in order_of_blocks]
    places = {}
    for place, j in enumerate(order_of_blocks):
        places[j] = place * share + place // max(1, blocks // 4) * SUB
    rows = min(side, 4 * SUB)
    signs = [parity_sign(jnp.bitwise_and(own, c), log2(blocks)) for c in range(chunks)]
    for start in range(0, side, rows):
        levels = [out[c * side + start : c * side + start + rows, :] for c in range(chunks)]
        if blocks == chunks:
            levels = [levels[0]] + [signs[c] * levels[c] for c in range(1, chunks)]
        for stride in strides:
            levels = butterfly(levels, stride)
        for c in range(chunks):
            if blocks == chunks:
                messages[places[c] + start : places[c] + start + rows, :] = levels[c]
            else:
                out[c * side + start : c * side + start + rows, :] = levels[c]
    if blocks != chunks:
        for j in range(blocks):
            source = pl.multiple_of(jnp.bitwise_xor(own, j) * share, share)
            messages[places[j] : places[j] + share, :] = out[pl.ds(source, share), :]
    quarter = messages.shape[0] // 4
    for k in range(4):
        messages[(k + 1) * quarter - SUB : (k + 1) * quarter, :] = total


def transform_local(amplitudes, qubit_order, row_axis):
    parts, unmeasured, length = amplitudes.shape
    chunks = length // CHUNK
    side = ROW_SIDE * ROW_SIDE
    count = qubit_order.shape[0]
    return pl.pallas_call(
        functools.partial(transform_kernel, row_axis),
        out_shape=pltpu.VMEM((chunks * side + 4 * SUB, LANES), jnp.float32),
        in_specs=[pl.BlockSpec(memory_space=pl.ANY), pl.BlockSpec(memory_space=pl.ANY)],
        out_specs=pl.BlockSpec(memory_space=pltpu.VMEM),
        scratch_shapes=[
            pltpu.VMEM((parts, unmeasured, length), jnp.float32),
            pltpu.VMEM((chunks * side, LANES), jnp.float32),
            pltpu.VMEM((ROW_SIDE, ROW_SIDE, LANES), jnp.float32),
            pltpu.VMEM((2 * LANES, LANES), jnp.bfloat16),
            pltpu.SMEM((count,), jnp.int32),
            *[pltpu.SMEM((count + 1,), jnp.int32) for _ in range(6)],
            pltpu.SemaphoreType.DMA(()),
            pltpu.SemaphoreType.DMA((2 * chunks, parts)),
        ],
        name="transform_local",
    )(qubit_order, amplitudes)


def exchange(message, axis, mask):
    size = lax.axis_size(axis)
    return lax.ppermute(message, axis, [(i, i ^ mask) for i in range(size)])


def sum_over_row(messages):
    for position in range(log2(lax.axis_size("row"))):
        half = messages.shape[0] // 2
        if position < 2:
            kept, sent = messages[:half], messages[half:]
        else:
            half = half - SUB // 2
            kept = jnp.concatenate([messages[:half], messages[-SUB:]])
            sent = messages[half:]
        messages = kept + exchange(sent, "row", 1 << position)
    return messages[:-SUB], messages[-SUB:]


def sign_of(axis, position):
    return 1.0 - 2.0 * bit_of(lax.axis_index(axis), position).astype(jnp.float32)


def butterflies(values, mass):
    left = list(range(log2(lax.axis_size("col"))))
    while left:
        bits, left = left[:2], left[2:]
        message = jnp.concatenate([values, mass])
        signs = [sign_of("col", b) for b in bits]
        new_values, new_mass = None, None
        for pick in reversed(range(1 << len(bits))):
            mask = sum(1 << b for k, b in enumerate(bits) if pick >> k & 1)
            received = message if mask == 0 else exchange(message, "col", mask)
            part, part_mass = received[:-SUB], received[-SUB:]
            for k in range(len(bits)):
                if not pick >> k & 1:
                    part = part * signs[k]
            new_values = part if new_values is None else new_values + part
            new_mass = part_mass if new_mass is None else new_mass + part_mass
        values, mass = new_values, new_mass
    return values, mass


def local(amplitudes, qubit_order, measured_qubits):
    values, mass = butterflies(*sum_over_row(transform_local(amplitudes, qubit_order, "row")))
    total = mass[:1]
    return (values * 2.0 ** (measured_qubits / 2) / total).reshape(1, -1)


def solution(mesh):
    def program(amplitudes, qubit_order):
        measured_qubits = log2(amplitudes.shape[2])
        return jax.shard_map(
            lambda a, q: local(a, q, measured_qubits),
            mesh=mesh,
            in_specs=(P(None, "row", "col"), P()),
            out_specs=P("col", "row"),
            check_vma=False,
        )(amplitudes, qubit_order)

    return program
```

```python
import functools

import jax
import jax.numpy as jnp
from jax import lax
from jax.experimental import pallas as pl
from jax.experimental.pallas import tpu as pltpu
from jax.sharding import PartitionSpec as P


LANES = 128
FIRST_PART = 6
SUB = 8
ROW_SIDE = 16
CHUNK = ROW_SIDE * ROW_SIDE * LANES


def log2(n):
    return n.bit_length() - 1


def parity_sign(common, bits):
    shift = 1
    while shift < bits:
        common = jnp.bitwise_xor(common, jnp.right_shift(common, shift))
        shift *= 2
    return (1 - 2 * jnp.bitwise_and(common, 1)).astype(jnp.float32)


def first_rows(share):
    unit = 4 * SUB if share % (8 * SUB) == 0 else SUB
    return share * FIRST_PART // 8 // unit * unit


def iota(shape, axis):
    return lax.broadcasted_iota(jnp.int32, shape, axis)


def bit_of(values, position):
    return jnp.bitwise_and(jnp.right_shift(values, position), 1)


def split(values):
    high = values.astype(jnp.bfloat16)
    low = (values - high.astype(jnp.float32)).astype(jnp.bfloat16)
    return jnp.concatenate([high, low], axis=1)


def transform_kernel(
    row_axis, order_in, amps, messages, buf, out, xs, hlane,
    order, inverse, rows_moved, lanes_moved, row_target, row_unit, lane_unit, order_sem, sems,
):
    parts, groups, length = buf.shape[0], buf.shape[1] // SUB, buf.shape[2]
    chunks = length // CHUNK
    half = CHUNK // 2
    side = ROW_SIDE * ROW_SIDE
    lane_bits, row_bits = log2(LANES), log2(ROW_SIDE)
    count = order.shape[0]

    def copies(step):
        return [
            pltpu.make_async_copy(
                amps.at[p, :, pl.ds(step * half, half)], buf.at[p, :, pl.ds(step * half, half)], sems.at[step, p]
            )
            for p in range(parts)
        ]

    order_copy = pltpu.make_async_copy(order_in, order, order_sem)
    order_copy.start()
    for step in range(2 * chunks):
        for copy in copies(step):
            copy.start()

    stacked = (2 * LANES, LANES)
    lane_sign = parity_sign(
        jnp.bitwise_and(jnp.bitwise_and(iota(stacked, 0), LANES - 1), iota(stacked, 1)), lane_bits
    )
    hlane[...] = lane_sign.astype(jnp.bfloat16)
    for p in range(count + 1):
        rows_moved[p] = lane_bits
        lanes_moved[p] = 0
    for r in range(row_bits + 1):
        lane_unit[r] = 0
    order_copy.wait()

    for j in range(count):
        inverse[order[j]] = j
    rank = jnp.int32(0)
    for p in range(lane_bits):
        lanes_moved[rank] = p
        rank = rank + (inverse[p] >= lane_bits).astype(jnp.int32)
    lane = iota((1, LANES), 1)
    lane_index = row_flip = out_row_flip = jnp.zeros((1, LANES), jnp.int32)
    rank = jnp.int32(0)
    for p in range(lane_bits, count):
        goes_to = inverse[p]
        crosses = goes_to < lane_bits
        rows_moved[rank] = p
        target = inverse[jnp.where(crosses, lanes_moved[rank], p)] - lane_bits
        row_target[p - lane_bits] = target
        row_unit[target] = 1 << p - lane_bits
        flip = jnp.left_shift(bit_of(lane, jnp.where(crosses, goes_to, 0)), target)
        out_row_flip = out_row_flip + jnp.where(crosses, flip, 0)
        rank = rank + crosses.astype(jnp.int32)
    rank = jnp.int32(0)
    for p in range(lane_bits):
        crosses = inverse[p] >= lane_bits
        partner = rows_moved[rank]
        lane_index = lane_index + jnp.left_shift(bit_of(lane, inverse[jnp.where(crosses, partner, p)]), p)
        target = row_target[jnp.where(crosses, partner - lane_bits, 0)]
        row_flip = row_flip + jnp.where(crosses, jnp.left_shift(bit_of(lane, p), target), 0)
        lane_unit[jnp.where(crosses, target, row_bits)] = 1 << p
        rank = rank + crosses.astype(jnp.int32)

    flips = [bit_of(row_flip, r) == 1 for r in range(row_bits)]
    out_flips = [bit_of(out_row_flip, r) == 1 for r in range(row_bits)]
    sources, gathers = [jnp.int32(0)], [jnp.int32(0)]
    for r in range(row_bits):
        sources = sources + [source + row_unit[r] for source in sources]
        gathers = gathers + [gather + lane_unit[r] for gather in gathers]
    gathers = [jnp.broadcast_to(jnp.bitwise_xor(lane_index, gather), (ROW_SIDE, LANES)) for gather in gathers]

    sub = iota((SUB, LANES), 0)
    masks = [bit_of(sub, level) == 0 for level in range(log2(SUB))]

    def packed_row(base, i):
        tiles = []
        for s in range(SUB):
            start = base + (s * ROW_SIDE + i) * LANES
            total = None
            for p in range(parts):
                for g in range(groups):
                    v = buf[p, g * SUB : (g + 1) * SUB, pl.ds(start, LANES)]
                    total = v * v if total is None else total + v * v
            tiles.append(total)
        for level in range(log2(SUB)):
            merged = []
            for k in range(0, len(tiles), 2):
                a, b = tiles[k] + tiles[k + 1], tiles[k] - tiles[k + 1]
                here = jnp.where(masks[level], a, b)
                other = jnp.where(masks[level], b, a)
                merged.append(here + pltpu.roll(other, SUB - (1 << level), 0))
            tiles = merged
        return tiles[0]

    def flip_rows(rows, which):
        for r in range(row_bits):
            rows = [jnp.where(which[r], rows[i ^ 1 << r], rows[i]) for i in range(ROW_SIDE)]
        return rows

    def butterfly(blocks, stride):
        return [
            blocks[c ^ stride] - blocks[c] if c & stride else blocks[c] + blocks[c ^ stride] for c in range(len(blocks))
        ]

    def arrive(step):
        for copy in copies(step):
            copy.wait()

    def sums(step, upper, total):
        base = pl.multiple_of(step * half, half)
        for i in range(ROW_SIDE):
            packed = packed_row(base, i)
            total = total + packed
            xs[i, upper * SUB : (upper + 1) * SUB, :] = packed
        return total

    def transform(c):
        rows = flip_rows([xs[source] for source in sources], flips)
        rows = [jnp.take_along_axis(rows[i], gathers[i], axis=1) for i in range(ROW_SIDE)]
        rows = flip_rows(rows, out_flips)
        for r in range(row_bits):
            rows = butterfly(rows, 1 << r)
        rows = [
            jnp.concatenate(butterfly([row[upper * SUB : (upper + 1) * SUB] for upper in range(2)], 1), axis=0)
            for row in rows
        ]
        z = jnp.dot(split(jnp.concatenate(rows, axis=0)), hlane[...], preferred_element_type=jnp.float32)
        first = pl.multiple_of(c * side, side)
        for i in range(ROW_SIDE):
            out[pl.ds(first + i, ROW_SIDE, stride=ROW_SIDE), :] = z[i * ROW_SIDE : (i + 1) * ROW_SIDE]

    def one_chunk(c, total):
        arrive(2 * c)
        transform(c - 1)
        total = sums(2 * c, 0, total)
        arrive(2 * c + 1)
        return sums(2 * c + 1, 1, total)

    total = jnp.zeros((SUB, LANES), jnp.float32)
    for upper in range(2):
        arrive(upper)
        total = sums(upper, upper, total)
    total = lax.fori_loop(1, chunks, one_chunk, total)
    transform(chunks - 1)
    total = jnp.broadcast_to(jnp.sum(total[:1], keepdims=True), (SUB, LANES))

    blocks = lax.axis_size(row_axis)
    share = out.shape[0] // blocks
    own = lax.axis_index(row_axis)
    order_of_blocks = [0]
    for k in reversed(range(log2(blocks))):
        order_of_blocks = order_of_blocks + [j + (1 << k) for j in order_of_blocks]
    first = first_rows(share)
    group = max(1, blocks // 4)
    quarter = messages.shape[0] // (blocks // group)

    def place(j, row):
        at = order_of_blocks.index(j)
        start = at // group * quarter
        if row < first:
            return start + at % group * first + row
        return start + group * first + SUB + at % group * (share - first) + row - first

    signs = [parity_sign(jnp.bitwise_and(own, c), log2(blocks)) for c in range(chunks)]
    rows = 4 * SUB
    for start in range(0, side, rows):
        levels = [out[c * side + start : c * side + start + rows, :] for c in range(chunks)]
        if blocks == chunks:
            levels = [levels[0]] + [signs[c] * levels[c] for c in range(1, chunks)]
        for k in range(log2(chunks)):
            levels = butterfly(levels, 1 << k)
        for c in range(chunks):
            if blocks == chunks:
                messages[place(c, start) : place(c, start) + rows, :] = levels[c]
            else:
                out[c * side + start : c * side + start + rows, :] = levels[c]
    if blocks != chunks:
        for j in range(blocks):
            source = jnp.bitwise_xor(own, j) * share
            for low, size in ((0, first), (first, share - first)):
                rows_in = pl.ds(pl.multiple_of(source + low, SUB), size)
                messages[place(j, low) : place(j, low) + size, :] = out[rows_in, :]
    for k in range(blocks // group):
        at = k * quarter + group * first
        messages[at : at + SUB, :] = total


def transform_local(amplitudes, qubit_order, row_axis):
    parts, unmeasured, length = amplitudes.shape
    chunks = length // CHUNK
    side = ROW_SIDE * ROW_SIDE
    count = qubit_order.shape[0]
    return pl.pallas_call(
        functools.partial(transform_kernel, row_axis),
        out_shape=pltpu.VMEM((chunks * side + min(4, lax.axis_size(row_axis)) * SUB, LANES), jnp.float32),
        in_specs=[pl.BlockSpec(memory_space=pl.ANY), pl.BlockSpec(memory_space=pl.ANY)],
        out_specs=pl.BlockSpec(memory_space=pltpu.VMEM),
        scratch_shapes=[
            pltpu.VMEM((parts, unmeasured, length), jnp.float32),
            pltpu.VMEM((chunks * side, LANES), jnp.float32),
            pltpu.VMEM((ROW_SIDE, ROW_SIDE, LANES), jnp.float32),
            pltpu.VMEM((2 * LANES, LANES), jnp.bfloat16),
            pltpu.SMEM((count,), jnp.int32),
            *[pltpu.SMEM((count + 1,), jnp.int32) for _ in range(6)],
            pltpu.SemaphoreType.DMA(()),
            pltpu.SemaphoreType.DMA((2 * chunks, parts)),
        ],
        name="transform_local",
    )(qubit_order, amplitudes)


def exchange(message, row_mask, col_mask):
    rows, cols = lax.axis_size("row"), lax.axis_size("col")
    mask = row_mask * cols + col_mask
    return lax.ppermute(message, ("row", "col"), [(i, i ^ mask) for i in range(rows * cols)])


def halve(message, tail):
    half = (message.shape[0] - tail) // 2
    if tail == 0:
        return message[:half], message[half:]
    return jnp.concatenate([message[:half], message[-tail:]]), message[half:]


def transform_step(kept, sent, row_mask, bits, tail):
    terms = []
    for pick in range(1 << len(bits)):
        mask = sum(1 << b for k, b in enumerate(bits) if pick >> k & 1)
        term = kept if mask == 0 else exchange(kept, 0, mask)
        if row_mask:
            term = term + exchange(sent, row_mask, mask)
        terms.append((pick, term))
    signs = [1.0 - 2.0 * bit_of(lax.axis_index("col"), b).astype(jnp.float32) for b in bits]
    rows = kept.shape[0] - tail
    values, summed = None, None
    for pick, term in reversed(terms):
        part = term[:rows]
        for k in range(len(bits)):
            if not pick >> k & 1:
                part = part * signs[k]
        values = part if values is None else values + part
        if tail:
            summed = term[rows:] if summed is None else summed + term[rows:]
    return jnp.concatenate([values, summed]) if tail else values


def run_steps(kept, sent, steps, tail):
    for number, (row_mask, bits) in enumerate(steps):
        if row_mask and number > 0:
            kept, sent = halve(kept, tail)
        kept = transform_step(kept, sent, row_mask, bits, tail)
    return kept


def local(amplitudes, qubit_order, measured_qubits):
    messages = transform_local(amplitudes, qubit_order, "row")
    row_bits, col_bits = log2(lax.axis_size("row")), log2(lax.axis_size("col"))
    half = messages.shape[0] // 2
    joined = messages[:half] + exchange(messages[half:], 1, 0)
    quarter = half // 2
    share = (messages.shape[0] - 4 * SUB) >> row_bits
    cut = (first_rows(share) << row_bits) // 4 + SUB

    rows = [(1 << k, []) for k in range(1, row_bits)]
    cols = list(range(col_bits))
    pairs = [(0, cols[k : k + 2]) for k in range(0, col_bits - 1, 2)]
    first_steps = rows + pairs + [(0, cols[-1:])] * (col_bits % 2)
    second_steps = rows[:-1] + [(rows[-1][0], cols[-1:] * (col_bits % 2))] + pairs
    first = run_steps(joined[:cut], joined[quarter : quarter + cut], first_steps, SUB)
    second = run_steps(joined[cut:quarter], joined[quarter + cut :], second_steps, 0)
    total = first[-SUB : 1 - SUB]
    values = jnp.concatenate([first[:-SUB], second])
    return (values * 2.0 ** (measured_qubits / 2) / total).reshape(1, -1)


def solution(mesh):
    def program(amplitudes, qubit_order):
        measured_qubits = log2(amplitudes.shape[2])
        return jax.shard_map(
            lambda a, q: local(a, q, measured_qubits),
            mesh=mesh,
            in_specs=(P(None, "row", "col"), P()),
            out_specs=P("col", "row"),
            check_vma=False,
        )(amplitudes, qubit_order)

    return program
```

```python
import functools

import jax
import jax.numpy as jnp
from jax import lax
from jax.experimental import pallas as pl
from jax.experimental.pallas import tpu as pltpu
from jax.sharding import PartitionSpec as P


LANES = 128
FIRST_PART = 5
SUB = 8
ROW_SIDE = 16
CHUNK = ROW_SIDE * ROW_SIDE * LANES


def log2(n):
    return n.bit_length() - 1


def parity_sign(common, bits):
    shift = 1
    while shift < bits:
        common = jnp.bitwise_xor(common, jnp.right_shift(common, shift))
        shift *= 2
    return (1 - 2 * jnp.bitwise_and(common, 1)).astype(jnp.float32)


def first_rows(share):
    unit = 4 * SUB if share % (8 * SUB) == 0 else SUB
    return share * FIRST_PART // 8 // unit * unit


def block_order(count):
    order = [0]
    for k in reversed(range(log2(count))):
        order = order + [j + (1 << k) for j in order]
    return order


def iota(shape, axis):
    return lax.broadcasted_iota(jnp.int32, shape, axis)


def bit_of(values, position):
    return jnp.bitwise_and(jnp.right_shift(values, position), 1)


def split(values):
    high = values.astype(jnp.bfloat16)
    low = (values - high.astype(jnp.float32)).astype(jnp.bfloat16)
    return jnp.concatenate([high, low], axis=1)


def transform_kernel(
    row_axis, order_in, amps, messages, buf, out, xs, hlane,
    order, inverse, rows_moved, lanes_moved, row_target, row_unit, lane_unit, order_sem, sems,
):
    parts, groups, length = buf.shape[0], buf.shape[1] // SUB, buf.shape[2]
    chunks = length // CHUNK
    half = CHUNK // 2
    side = ROW_SIDE * ROW_SIDE
    lane_bits, row_bits = log2(LANES), log2(ROW_SIDE)
    count = order.shape[0]

    def copies(step):
        return [
            pltpu.make_async_copy(
                amps.at[p, :, pl.ds(step * half, half)], buf.at[p, :, pl.ds(step * half, half)], sems.at[step, p]
            )
            for p in range(parts)
        ]

    order_copy = pltpu.make_async_copy(order_in, order, order_sem)
    order_copy.start()
    for step in range(2 * chunks):
        for copy in copies(step):
            copy.start()

    stacked = (2 * LANES, LANES)
    lane_sign = parity_sign(
        jnp.bitwise_and(jnp.bitwise_and(iota(stacked, 0), LANES - 1), iota(stacked, 1)), lane_bits
    )
    hlane[...] = lane_sign.astype(jnp.bfloat16)
    for p in range(count + 1):
        rows_moved[p] = lane_bits
        lanes_moved[p] = 0
    for r in range(row_bits + 1):
        lane_unit[r] = 0
    order_copy.wait()

    for j in range(count):
        inverse[order[j]] = j
    rank = jnp.int32(0)
    for p in range(lane_bits):
        lanes_moved[rank] = p
        rank = rank + (inverse[p] >= lane_bits).astype(jnp.int32)
    lane = iota((1, LANES), 1)
    lane_index = row_flip = out_row_flip = jnp.zeros((1, LANES), jnp.int32)
    rank = jnp.int32(0)
    for p in range(lane_bits, count):
        goes_to = inverse[p]
        crosses = goes_to < lane_bits
        rows_moved[rank] = p
        target = inverse[jnp.where(crosses, lanes_moved[rank], p)] - lane_bits
        row_target[p - lane_bits] = target
        row_unit[target] = 1 << p - lane_bits
        flip = jnp.left_shift(bit_of(lane, jnp.where(crosses, goes_to, 0)), target)
        out_row_flip = out_row_flip + jnp.where(crosses, flip, 0)
        rank = rank + crosses.astype(jnp.int32)
    rank = jnp.int32(0)
    for p in range(lane_bits):
        crosses = inverse[p] >= lane_bits
        partner = rows_moved[rank]
        lane_index = lane_index + jnp.left_shift(bit_of(lane, inverse[jnp.where(crosses, partner, p)]), p)
        target = row_target[jnp.where(crosses, partner - lane_bits, 0)]
        row_flip = row_flip + jnp.where(crosses, jnp.left_shift(bit_of(lane, p), target), 0)
        lane_unit[jnp.where(crosses, target, row_bits)] = 1 << p
        rank = rank + crosses.astype(jnp.int32)

    flips = [bit_of(row_flip, r) == 1 for r in range(row_bits)]
    out_flips = [bit_of(out_row_flip, r) == 1 for r in range(row_bits)]
    sources, gathers = [jnp.int32(0)], [jnp.int32(0)]
    for r in range(row_bits):
        sources = sources + [source + row_unit[r] for source in sources]
        gathers = gathers + [gather + lane_unit[r] for gather in gathers]
    gathers = [jnp.broadcast_to(jnp.bitwise_xor(lane_index, gather), (ROW_SIDE, LANES)) for gather in gathers]

    sub = iota((SUB, LANES), 0)
    masks = [bit_of(sub, level) == 0 for level in range(log2(SUB))]

    def packed_row(base, i):
        tiles = []
        for s in range(SUB):
            start = base + (s * ROW_SIDE + i) * LANES
            total = None
            for p in range(parts):
                for g in range(groups):
                    v = buf[p, g * SUB : (g + 1) * SUB, pl.ds(start, LANES)]
                    total = v * v if total is None else total + v * v
            tiles.append(total)
        for level in range(log2(SUB)):
            merged = []
            for k in range(0, len(tiles), 2):
                a, b = tiles[k] + tiles[k + 1], tiles[k] - tiles[k + 1]
                here = jnp.where(masks[level], a, b)
                other = jnp.where(masks[level], b, a)
                merged.append(here + pltpu.roll(other, SUB - (1 << level), 0))
            tiles = merged
        return tiles[0]

    def flip_rows(rows, which):
        for r in range(row_bits):
            rows = [jnp.where(which[r], rows[i ^ 1 << r], rows[i]) for i in range(ROW_SIDE)]
        return rows

    def butterfly(blocks, stride):
        return [
            blocks[c ^ stride] - blocks[c] if c & stride else blocks[c] + blocks[c ^ stride] for c in range(len(blocks))
        ]

    def arrive(step):
        for copy in copies(step):
            copy.wait()

    def sums(step, upper, total):
        base = pl.multiple_of(step * half, half)
        for i in range(ROW_SIDE):
            packed = packed_row(base, i)
            total = total + packed
            xs[i, upper * SUB : (upper + 1) * SUB, :] = packed
        return total

    def transform(c):
        rows = flip_rows([xs[source] for source in sources], flips)
        rows = [jnp.take_along_axis(rows[i], gathers[i], axis=1) for i in range(ROW_SIDE)]
        rows = flip_rows(rows, out_flips)
        for r in range(row_bits):
            rows = butterfly(rows, 1 << r)
        rows = [
            jnp.concatenate(butterfly([row[upper * SUB : (upper + 1) * SUB] for upper in range(2)], 1), axis=0)
            for row in rows
        ]
        z = jnp.dot(split(jnp.concatenate(rows, axis=0)), hlane[...], preferred_element_type=jnp.float32)
        first = pl.multiple_of(c * side, side)
        for i in range(ROW_SIDE):
            out[pl.ds(first + i, ROW_SIDE, stride=ROW_SIDE), :] = z[i * ROW_SIDE : (i + 1) * ROW_SIDE]

    def one_chunk(c, total):
        arrive(2 * c)
        transform(c - 1)
        total = sums(2 * c, 0, total)
        arrive(2 * c + 1)
        return sums(2 * c + 1, 1, total)

    total = jnp.zeros((SUB, LANES), jnp.float32)
    for upper in range(2):
        arrive(upper)
        total = sums(upper, upper, total)
    total = lax.fori_loop(1, chunks, one_chunk, total)
    transform(chunks - 1)
    total = jnp.broadcast_to(jnp.sum(total[:1], keepdims=True), (SUB, LANES))

    blocks = lax.axis_size(row_axis)
    share = out.shape[0] // blocks
    own = lax.axis_index(row_axis)
    order_of_blocks = block_order(blocks)
    first = first_rows(share)

    def place(j, row):
        at = order_of_blocks.index(j)
        if row < first:
            return at * (first + SUB) + row
        return blocks * (first + SUB) + at * (share - first) + row - first

    signs = [parity_sign(jnp.bitwise_and(own, c), log2(blocks)) for c in range(chunks)]
    rows = 4 * SUB
    for start in range(0, side, rows):
        levels = [out[c * side + start : c * side + start + rows, :] for c in range(chunks)]
        if blocks == chunks:
            levels = [levels[0]] + [signs[c] * levels[c] for c in range(1, chunks)]
        for k in range(log2(chunks)):
            levels = butterfly(levels, 1 << k)
        for c in range(chunks):
            if blocks == chunks:
                messages[place(c, start) : place(c, start) + rows, :] = levels[c]
            else:
                out[c * side + start : c * side + start + rows, :] = levels[c]
    if blocks != chunks:
        for j in range(blocks):
            source = jnp.bitwise_xor(own, j) * share
            for low, size in ((0, first), (first, share - first)):
                rows_in = pl.ds(pl.multiple_of(source + low, SUB), size)
                messages[place(j, low) : place(j, low) + size, :] = out[rows_in, :]
    for k in range(blocks):
        at = k * (first + SUB) + first
        messages[at : at + SUB, :] = total


def transform_local(amplitudes, qubit_order, row_axis):
    parts, unmeasured, length = amplitudes.shape
    chunks = length // CHUNK
    side = ROW_SIDE * ROW_SIDE
    count = qubit_order.shape[0]
    return pl.pallas_call(
        functools.partial(transform_kernel, row_axis),
        out_shape=pltpu.VMEM((chunks * side + lax.axis_size(row_axis) * SUB, LANES), jnp.float32),
        in_specs=[pl.BlockSpec(memory_space=pl.ANY), pl.BlockSpec(memory_space=pl.ANY)],
        out_specs=pl.BlockSpec(memory_space=pltpu.VMEM),
        scratch_shapes=[
            pltpu.VMEM((parts, unmeasured, length), jnp.float32),
            pltpu.VMEM((chunks * side, LANES), jnp.float32),
            pltpu.VMEM((ROW_SIDE, ROW_SIDE, LANES), jnp.float32),
            pltpu.VMEM((2 * LANES, LANES), jnp.bfloat16),
            pltpu.SMEM((count,), jnp.int32),
            *[pltpu.SMEM((count + 1,), jnp.int32) for _ in range(6)],
            pltpu.SemaphoreType.DMA(()),
            pltpu.SemaphoreType.DMA((2 * chunks, parts)),
        ],
        name="transform_local",
    )(qubit_order, amplitudes)


def exchange(message, row_mask, col_mask):
    rows, cols = lax.axis_size("row"), lax.axis_size("col")
    mask = row_mask * cols + col_mask
    return lax.ppermute(message, ("row", "col"), [(i, i ^ mask) for i in range(rows * cols)])


def pick_of(bits, pick):
    return sum(1 << b for k, b in enumerate(bits) if pick >> k & 1)


def run_steps(blocks, steps, tail):
    for row_bits, col_bits in steps:
        dropped = pick_of(row_bits, -1)
        left = [j for j in blocks if j & dropped == 0]
        size = blocks[0].shape[0]
        signs = [1.0 - 2.0 * bit_of(lax.axis_index("col"), b).astype(jnp.float32) for b in col_bits]
        terms = []
        for row_pick in range(1 << len(row_bits)):
            row_mask = pick_of(row_bits, row_pick)
            joined = [blocks[j ^ row_mask] for j in left]
            message = joined[0] if len(joined) == 1 else jnp.concatenate(joined)
            for pick in range(1 << len(col_bits)):
                col_mask = pick_of(col_bits, pick)
                term = message
                if row_mask or col_mask:
                    term = exchange(message, row_mask, col_mask)
                terms.append((pick, term))
        blocks = {}
        for k, j in enumerate(left):
            values, summed = None, None
            for pick, term in terms:
                term = term[k * size : (k + 1) * size]
                part = term[: size - tail] if col_bits else term
                for n in range(len(col_bits)):
                    if not pick >> n & 1:
                        part = part * signs[n]
                values = part if values is None else values + part
                if tail and col_bits:
                    summed = term[size - tail :] if summed is None else summed + term[size - tail :]
            blocks[j] = jnp.concatenate([values, summed]) if tail and col_bits else values
    return blocks[0]


def local(amplitudes, qubit_order, measured_qubits):
    messages = transform_local(amplitudes, qubit_order, "row")
    count = lax.axis_size("row")
    row_bits, col_bits = log2(count), log2(lax.axis_size("col"))
    share = messages.shape[0] // count - SUB
    first = first_rows(share)
    first_blocks, second_blocks = {}, {}
    order_of_blocks = block_order(count)
    for at, j in enumerate(order_of_blocks):
        first_blocks[j] = messages[at * (first + SUB) : (at + 1) * (first + SUB)]
        start = count * (first + SUB) + at * (share - first)
        second_blocks[j] = messages[start : start + share - first]

    later = [((k,), ()) for k in range(2, row_bits)]
    first_steps = [((0,), ()), ((1,), (0,))] + later + [((), (b,)) for b in range(1, col_bits)]
    others = list(range(col_bits - 1))
    second_steps = [((0, 1), ())] + later + [((), (col_bits - 1,))]
    second_steps += [((), tuple(others[k : k + 2])) for k in range(0, len(others), 2)]
    one = run_steps(first_blocks, first_steps, SUB)
    two = run_steps(second_blocks, second_steps, 0)
    total = one[-SUB : 1 - SUB]
    values = jnp.concatenate([one[:-SUB], two])
    return (values * 2.0 ** (measured_qubits / 2) / total).reshape(1, -1)


def solution(mesh):
    def program(amplitudes, qubit_order):
        measured_qubits = log2(amplitudes.shape[2])

        def body(a, q):
            return local(a, q, measured_qubits)

        return jax.shard_map(
            body,
            mesh=mesh,
            in_specs=(P(None, "row", "col"), P()),
            out_specs=P("col", "row"),
            check_vma=False,
        )(amplitudes, qubit_order)

    return program
```

```python
import functools

import jax
import jax.numpy as jnp
from jax import lax
from jax.experimental import pallas as pl
from jax.experimental.pallas import tpu as pltpu
from jax.sharding import PartitionSpec as P


LANES = 128
FIRST_PART = 5
SUB = 8
ROW_SIDE = 16
CHUNK = ROW_SIDE * ROW_SIDE * LANES


def log2(n):
    return n.bit_length() - 1


def parity_sign(common, bits):
    shift = 1
    while shift < bits:
        common = jnp.bitwise_xor(common, jnp.right_shift(common, shift))
        shift *= 2
    return (1 - 2 * jnp.bitwise_and(common, 1)).astype(jnp.float32)


def first_rows(share):
    unit = 4 * SUB if share % (8 * SUB) == 0 else SUB
    return share * FIRST_PART // 8 // unit * unit


def block_order(count):
    order = [0]
    for k in reversed(range(log2(count))):
        order = order + [j + (1 << k) for j in order]
    return order


def iota(shape, axis):
    return lax.broadcasted_iota(jnp.int32, shape, axis)


def bit_of(values, position):
    return jnp.bitwise_and(jnp.right_shift(values, position), 1)


def split(values):
    high = values.astype(jnp.bfloat16)
    low = (values - high.astype(jnp.float32)).astype(jnp.bfloat16)
    return jnp.concatenate([high, low], axis=1)


def transform_kernel(
    row_axis, order_in, amps, messages, buf, out, xs, hlane, row_signs,
    order, inverse, rows_moved, lanes_moved, row_target, row_unit, lane_unit, order_sem, sems,
):
    parts, groups, length = buf.shape[0], buf.shape[1] // SUB, buf.shape[2]
    chunks = length // CHUNK
    half = CHUNK // 2
    side = ROW_SIDE * ROW_SIDE
    lane_bits, row_bits = log2(LANES), log2(ROW_SIDE)
    count = order.shape[0]

    def copies(step):
        return [
            pltpu.make_async_copy(
                amps.at[p, :, pl.ds(step * half, half)], buf.at[p, :, pl.ds(step * half, half)], sems.at[step, p]
            )
            for p in range(parts)
        ]

    order_copy = pltpu.make_async_copy(order_in, order, order_sem)
    order_copy.start()
    for step in range(2 * chunks):
        for copy in copies(step):
            copy.start()

    stacked = (2 * LANES, LANES)
    lane_sign = parity_sign(
        jnp.bitwise_and(jnp.bitwise_and(iota(stacked, 0), LANES - 1), iota(stacked, 1)), lane_bits
    )
    hlane[...] = lane_sign.astype(jnp.bfloat16)
    for p in range(count + 1):
        rows_moved[p] = lane_bits
        lanes_moved[p] = 0
    for r in range(row_bits + 1):
        lane_unit[r] = 0
    order_copy.wait()

    for j in range(count):
        inverse[order[j]] = j
    rank = jnp.int32(0)
    for p in range(lane_bits):
        lanes_moved[rank] = p
        rank = rank + (inverse[p] >= lane_bits).astype(jnp.int32)
    lane = iota((1, LANES), 1)
    lane_index = row_flip = out_row_flip = jnp.zeros((1, LANES), jnp.int32)
    rank = jnp.int32(0)
    for p in range(lane_bits, count):
        goes_to = inverse[p]
        crosses = goes_to < lane_bits
        rows_moved[rank] = p
        target = inverse[jnp.where(crosses, lanes_moved[rank], p)] - lane_bits
        row_target[p - lane_bits] = target
        row_unit[target] = 1 << p - lane_bits
        flip = jnp.left_shift(bit_of(lane, jnp.where(crosses, goes_to, 0)), target)
        out_row_flip = out_row_flip + jnp.where(crosses, flip, 0)
        rank = rank + crosses.astype(jnp.int32)
    rank = jnp.int32(0)
    for p in range(lane_bits):
        crosses = inverse[p] >= lane_bits
        partner = rows_moved[rank]
        lane_index = lane_index + jnp.left_shift(bit_of(lane, inverse[jnp.where(crosses, partner, p)]), p)
        target = row_target[jnp.where(crosses, partner - lane_bits, 0)]
        row_flip = row_flip + jnp.where(crosses, jnp.left_shift(bit_of(lane, p), target), 0)
        lane_unit[jnp.where(crosses, target, row_bits)] = 1 << p
        rank = rank + crosses.astype(jnp.int32)

    flips = [bit_of(row_flip, r) == 1 for r in range(row_bits)]
    row_signs[...] = parity_sign(jnp.bitwise_and(iota((ROW_SIDE, LANES), 0), out_row_flip), row_bits)
    sources, gathers = [jnp.int32(0)], [jnp.int32(0)]
    for r in range(row_bits):
        sources = sources + [source + row_unit[r] for source in sources]
        gathers = gathers + [gather + lane_unit[r] for gather in gathers]
    gathers = [jnp.broadcast_to(jnp.bitwise_xor(lane_index, gather), (ROW_SIDE, LANES)) for gather in gathers]

    sub = iota((SUB, LANES), 0)
    masks = [bit_of(sub, level) == 0 for level in range(log2(SUB))]

    def packed_row(base, i):
        tiles = []
        for s in range(SUB):
            start = base + (s * ROW_SIDE + i) * LANES
            total = None
            for p in range(parts):
                for g in range(groups):
                    v = buf[p, g * SUB : (g + 1) * SUB, pl.ds(start, LANES)]
                    total = v * v if total is None else total + v * v
            tiles.append(total)
        for level in range(log2(SUB)):
            merged = []
            for k in range(0, len(tiles), 2):
                a, b = tiles[k] + tiles[k + 1], tiles[k] - tiles[k + 1]
                here = jnp.where(masks[level], a, b)
                other = jnp.where(masks[level], b, a)
                merged.append(here + pltpu.roll(other, SUB - (1 << level), 0))
            tiles = merged
        return tiles[0]

    def butterfly(blocks, stride):
        return [
            blocks[c ^ stride] - blocks[c] if c & stride else blocks[c] + blocks[c ^ stride] for c in range(len(blocks))
        ]

    def arrive(step):
        for copy in copies(step):
            copy.wait()

    def sums(step, upper, total):
        base = pl.multiple_of(step * half, half)
        for i in range(ROW_SIDE):
            packed = packed_row(base, i)
            total = total + packed
            xs[i, upper * SUB : (upper + 1) * SUB, :] = packed
        return total

    def transform(c):
        rows = [xs[source] for source in sources]
        for r in range(row_bits):
            rows = [jnp.where(flips[r], rows[i ^ 1 << r], rows[i]) for i in range(ROW_SIDE)]
        rows = [jnp.take_along_axis(rows[i], gathers[i], axis=1) for i in range(ROW_SIDE)]
        for r in range(row_bits):
            rows = butterfly(rows, 1 << r)
        rows = [rows[i] * row_signs[i : i + 1, :] for i in range(ROW_SIDE)]
        rows = [
            jnp.concatenate(butterfly([row[upper * SUB : (upper + 1) * SUB] for upper in range(2)], 1), axis=0)
            for row in rows
        ]
        z = jnp.dot(split(jnp.concatenate(rows, axis=0)), hlane[...], preferred_element_type=jnp.float32)
        first = pl.multiple_of(c * side, side)
        for i in range(ROW_SIDE):
            out[pl.ds(first + i, ROW_SIDE, stride=ROW_SIDE), :] = z[i * ROW_SIDE : (i + 1) * ROW_SIDE]

    def one_chunk(c, total):
        transform(c - 1)
        arrive(2 * c)
        total = sums(2 * c, 0, total)
        arrive(2 * c + 1)
        return sums(2 * c + 1, 1, total)

    total = jnp.zeros((SUB, LANES), jnp.float32)
    for upper in range(2):
        arrive(upper)
        total = sums(upper, upper, total)
    total = lax.fori_loop(1, chunks, one_chunk, total)
    transform(chunks - 1)
    total = jnp.broadcast_to(jnp.sum(total[:1], keepdims=True), (SUB, LANES))

    blocks = lax.axis_size(row_axis)
    share = out.shape[0] // blocks
    own = lax.axis_index(row_axis)
    order_of_blocks = block_order(blocks)
    first = first_rows(share)

    def place(j, row):
        at = order_of_blocks.index(j)
        if row < first:
            return at * (first + SUB) + row
        return blocks * (first + SUB) + at * (share - first) + row - first

    signs = [parity_sign(jnp.bitwise_and(own, c), log2(blocks)) for c in range(chunks)]
    rows = 4 * SUB
    for start in range(0, side, rows):
        levels = [out[c * side + start : c * side + start + rows, :] for c in range(chunks)]
        if blocks == chunks:
            levels = [levels[0]] + [signs[c] * levels[c] for c in range(1, chunks)]
        for k in range(log2(chunks)):
            levels = butterfly(levels, 1 << k)
        for c in range(chunks):
            if blocks == chunks:
                messages[place(c, start) : place(c, start) + rows, :] = levels[c]
            else:
                out[c * side + start : c * side + start + rows, :] = levels[c]
    if blocks != chunks:
        for j in range(blocks):
            source = jnp.bitwise_xor(own, j) * share
            for low, size in ((0, first), (first, share - first)):
                rows_in = pl.ds(pl.multiple_of(source + low, SUB), size)
                messages[place(j, low) : place(j, low) + size, :] = out[rows_in, :]
    for k in range(blocks):
        at = k * (first + SUB) + first
        messages[at : at + SUB, :] = total


def transform_local(amplitudes, qubit_order, row_axis):
    parts, unmeasured, length = amplitudes.shape
    chunks = length // CHUNK
    side = ROW_SIDE * ROW_SIDE
    count = qubit_order.shape[0]
    return pl.pallas_call(
        functools.partial(transform_kernel, row_axis),
        out_shape=pltpu.VMEM((chunks * side + lax.axis_size(row_axis) * SUB, LANES), jnp.float32),
        in_specs=[pl.BlockSpec(memory_space=pl.ANY), pl.BlockSpec(memory_space=pl.ANY)],
        out_specs=pl.BlockSpec(memory_space=pltpu.VMEM),
        scratch_shapes=[
            pltpu.VMEM((parts, unmeasured, length), jnp.float32),
            pltpu.VMEM((chunks * side, LANES), jnp.float32),
            pltpu.VMEM((ROW_SIDE, ROW_SIDE, LANES), jnp.float32),
            pltpu.VMEM((2 * LANES, LANES), jnp.bfloat16),
            pltpu.VMEM((ROW_SIDE, LANES), jnp.float32),
            pltpu.SMEM((count,), jnp.int32),
            *[pltpu.SMEM((count + 1,), jnp.int32) for _ in range(6)],
            pltpu.SemaphoreType.DMA(()),
            pltpu.SemaphoreType.DMA((2 * chunks, parts)),
        ],
        name="transform_local",
    )(qubit_order, amplitudes)


def exchange(message, row_mask, col_mask):
    rows, cols = lax.axis_size("row"), lax.axis_size("col")
    mask = row_mask * cols + col_mask
    return lax.ppermute(message, ("row", "col"), [(i, i ^ mask) for i in range(rows * cols)])


def pick_of(bits, pick):
    return sum(1 << b for k, b in enumerate(bits) if pick >> k & 1)


def run_steps(blocks, steps, tail):
    for row_bits, col_bits in steps:
        dropped = pick_of(row_bits, -1)
        left = [j for j in blocks if j & dropped == 0]
        size = blocks[0].shape[0]
        signs = [1.0 - 2.0 * bit_of(lax.axis_index("col"), b).astype(jnp.float32) for b in col_bits]
        terms = []
        for row_pick in range(1 << len(row_bits)):
            row_mask = pick_of(row_bits, row_pick)
            joined = [blocks[j ^ row_mask] for j in left]
            message = joined[0] if len(joined) == 1 else jnp.concatenate(joined)
            for pick in range(1 << len(col_bits)):
                col_mask = pick_of(col_bits, pick)
                term = message
                if row_mask or col_mask:
                    term = exchange(message, row_mask, col_mask)
                terms.append((pick, term))
        blocks = {}
        for k, j in enumerate(left):
            values, summed = None, None
            for pick, term in terms:
                term = term[k * size : (k + 1) * size]
                part = term[: size - tail] if col_bits else term
                for n in range(len(col_bits)):
                    if not pick >> n & 1:
                        part = part * signs[n]
                values = part if values is None else values + part
                if tail and col_bits:
                    summed = term[size - tail :] if summed is None else summed + term[size - tail :]
            blocks[j] = jnp.concatenate([values, summed]) if tail and col_bits else values
    return blocks[0]


def local(amplitudes, qubit_order, measured_qubits):
    messages = transform_local(amplitudes, qubit_order, "row")
    count = lax.axis_size("row")
    row_bits, col_bits = log2(count), log2(lax.axis_size("col"))
    share = messages.shape[0] // count - SUB
    first = first_rows(share)
    first_blocks, second_blocks = {}, {}
    order_of_blocks = block_order(count)
    for at, j in enumerate(order_of_blocks):
        first_blocks[j] = messages[at * (first + SUB) : (at + 1) * (first + SUB)]
        start = count * (first + SUB) + at * (share - first)
        second_blocks[j] = messages[start : start + share - first]

    later = [((k,), ()) for k in range(2, row_bits)]
    first_steps = [((0,), ()), ((1,), (0,))] + later + [((), (b,)) for b in range(1, col_bits)]
    others = list(range(col_bits - 1))
    second_steps = [((0, 1), ())] + later + [((), (col_bits - 1,))]
    second_steps += [((), tuple(others[k : k + 2])) for k in range(0, len(others), 2)]
    one = run_steps(first_blocks, first_steps, SUB)
    two = run_steps(second_blocks, second_steps, 0)
    total = one[-SUB : 1 - SUB]
    values = jnp.concatenate([one[:-SUB], two])
    return (values * 2.0 ** (measured_qubits / 2) / total).reshape(1, -1)


def solution(mesh):
    def program(amplitudes, qubit_order):
        measured_qubits = log2(amplitudes.shape[2])

        def body(a, q):
            return local(a, q, measured_qubits)

        return jax.shard_map(
            body,
            mesh=mesh,
            in_specs=(P(None, "row", "col"), P()),
            out_specs=P("col", "row"),
            check_vma=False,
        )(amplitudes, qubit_order)

    return program
```

```python
import functools

import jax
import jax.numpy as jnp
from jax import lax
from jax.experimental import pallas as pl
from jax.experimental.pallas import tpu as pltpu
from jax.sharding import PartitionSpec as P


LANES = 128
FIRST_PART = 10
SUB = 8
ROW_SIDE = 16
CHUNK = ROW_SIDE * ROW_SIDE * LANES


def log2(n):
    return n.bit_length() - 1


def parity_sign(common, bits):
    shift = 1
    while shift < bits:
        common = jnp.bitwise_xor(common, jnp.right_shift(common, shift))
        shift *= 2
    return (1 - 2 * jnp.bitwise_and(common, 1)).astype(jnp.float32)


def first_rows(share):
    unit = 2 * SUB if share % (4 * SUB) == 0 else SUB
    return share * FIRST_PART // 16 // unit * unit


def block_order(count):
    order = [0]
    for k in reversed(range(log2(count))):
        order = order + [j + (1 << k) for j in order]
    return order


def iota(shape, axis):
    return lax.broadcasted_iota(jnp.int32, shape, axis)


def bit_of(values, position):
    return jnp.bitwise_and(jnp.right_shift(values, position), 1)


def split(values):
    high = values.astype(jnp.bfloat16)
    low = (values - high.astype(jnp.float32)).astype(jnp.bfloat16)
    return jnp.concatenate([high, low], axis=1)


def transform_kernel(
    row_axis, order_in, amps, messages, buf, out, xs, hlane, row_signs,
    order, inverse, rows_moved, lanes_moved, row_target, row_unit, lane_unit, order_sem, sems,
):
    parts, groups, length = buf.shape[0], buf.shape[1] // SUB, buf.shape[2]
    chunks = length // CHUNK
    half = CHUNK // 2
    side = ROW_SIDE * ROW_SIDE
    lane_bits, row_bits = log2(LANES), log2(ROW_SIDE)
    count = order.shape[0]

    def copies(step):
        return [
            pltpu.make_async_copy(
                amps.at[p, :, pl.ds(step * half, half)], buf.at[p, :, pl.ds(step * half, half)], sems.at[step, p]
            )
            for p in range(parts)
        ]

    order_copy = pltpu.make_async_copy(order_in, order, order_sem)
    order_copy.start()
    for step in range(2 * chunks):
        for copy in copies(step):
            copy.start()

    stacked = (2 * LANES, LANES)
    lane_sign = parity_sign(
        jnp.bitwise_and(jnp.bitwise_and(iota(stacked, 0), LANES - 1), iota(stacked, 1)), lane_bits
    )
    hlane[...] = lane_sign.astype(jnp.bfloat16)
    for p in range(count + 1):
        rows_moved[p] = lane_bits
        lanes_moved[p] = 0
    for r in range(row_bits + 1):
        lane_unit[r] = 0
    order_copy.wait()

    for j in range(count):
        inverse[order[j]] = j
    rank = jnp.int32(0)
    for p in range(lane_bits):
        lanes_moved[rank] = p
        rank = rank + (inverse[p] >= lane_bits).astype(jnp.int32)
    lane = iota((1, LANES), 1)
    lane_index = row_flip = out_row_flip = jnp.zeros((1, LANES), jnp.int32)
    rank = jnp.int32(0)
    for p in range(lane_bits, count):
        goes_to = inverse[p]
        crosses = goes_to < lane_bits
        rows_moved[rank] = p
        target = inverse[jnp.where(crosses, lanes_moved[rank], p)] - lane_bits
        row_target[p - lane_bits] = target
        row_unit[target] = 1 << p - lane_bits
        flip = jnp.left_shift(bit_of(lane, jnp.where(crosses, goes_to, 0)), target)
        out_row_flip = out_row_flip + jnp.where(crosses, flip, 0)
        rank = rank + crosses.astype(jnp.int32)
    rank = jnp.int32(0)
    for p in range(lane_bits):
        crosses = inverse[p] >= lane_bits
        partner = rows_moved[rank]
        lane_index = lane_index + jnp.left_shift(bit_of(lane, inverse[jnp.where(crosses, partner, p)]), p)
        target = row_target[jnp.where(crosses, partner - lane_bits, 0)]
        row_flip = row_flip + jnp.where(crosses, jnp.left_shift(bit_of(lane, p), target), 0)
        lane_unit[jnp.where(crosses, target, row_bits)] = 1 << p
        rank = rank + crosses.astype(jnp.int32)

    flips = [bit_of(row_flip, r) == 1 for r in range(row_bits)]
    row_signs[...] = parity_sign(jnp.bitwise_and(iota((ROW_SIDE, LANES), 0), out_row_flip), row_bits)
    sources, gathers = [jnp.int32(0)], [jnp.int32(0)]
    for r in range(row_bits):
        sources = sources + [source + row_unit[r] for source in sources]
        gathers = gathers + [gather + lane_unit[r] for gather in gathers]
    gathers = [jnp.broadcast_to(jnp.bitwise_xor(lane_index, gather), (ROW_SIDE, LANES)) for gather in gathers]

    sub = iota((SUB, LANES), 0)
    masks = [bit_of(sub, level) == 0 for level in range(log2(SUB))]

    def packed_row(base, i):
        tiles = []
        for s in range(SUB):
            start = base + (s * ROW_SIDE + i) * LANES
            total = None
            for p in range(parts):
                for g in range(groups):
                    v = buf[p, g * SUB : (g + 1) * SUB, pl.ds(start, LANES)]
                    total = v * v if total is None else total + v * v
            tiles.append(total)
        for level in range(log2(SUB)):
            merged = []
            for k in range(0, len(tiles), 2):
                a, b = tiles[k] + tiles[k + 1], tiles[k] - tiles[k + 1]
                here = jnp.where(masks[level], a, b)
                other = jnp.where(masks[level], b, a)
                merged.append(here + pltpu.roll(other, SUB - (1 << level), 0))
            tiles = merged
        return tiles[0]

    def butterfly(blocks, stride):
        return [
            blocks[c ^ stride] - blocks[c] if c & stride else blocks[c] + blocks[c ^ stride] for c in range(len(blocks))
        ]

    def arrive(step):
        for copy in copies(step):
            copy.wait()

    def sums(step, upper, total):
        base = pl.multiple_of(step * half, half)
        for i in range(ROW_SIDE):
            packed = packed_row(base, i)
            total = total + packed
            xs[i, upper * SUB : (upper + 1) * SUB, :] = packed
        return total

    def transform(c):
        rows = [xs[source] for source in sources]
        for r in range(row_bits):
            rows = [jnp.where(flips[r], rows[i ^ 1 << r], rows[i]) for i in range(ROW_SIDE)]
        rows = [jnp.take_along_axis(rows[i], gathers[i], axis=1) for i in range(ROW_SIDE)]
        for r in range(row_bits):
            rows = butterfly(rows, 1 << r)
        rows = [rows[i] * row_signs[i : i + 1, :] for i in range(ROW_SIDE)]
        rows = [
            jnp.concatenate(butterfly([row[upper * SUB : (upper + 1) * SUB] for upper in range(2)], 1), axis=0)
            for row in rows
        ]
        z = jnp.dot(split(jnp.concatenate(rows, axis=0)), hlane[...], preferred_element_type=jnp.float32)
        first = pl.multiple_of(c * side, side)
        for i in range(ROW_SIDE):
            out[pl.ds(first + i, ROW_SIDE, stride=ROW_SIDE), :] = z[i * ROW_SIDE : (i + 1) * ROW_SIDE]

    def one_chunk(c, total):
        transform(c - 1)
        arrive(2 * c)
        total = sums(2 * c, 0, total)
        arrive(2 * c + 1)
        return sums(2 * c + 1, 1, total)

    total = jnp.zeros((SUB, LANES), jnp.float32)
    for upper in range(2):
        arrive(upper)
        total = sums(upper, upper, total)
    total = lax.fori_loop(1, chunks, one_chunk, total)
    transform(chunks - 1)
    total = jnp.broadcast_to(jnp.sum(total[:1], keepdims=True), (SUB, LANES))

    blocks = lax.axis_size(row_axis)
    share = out.shape[0] // blocks
    own = lax.axis_index(row_axis)
    order_of_blocks = block_order(blocks)
    first = first_rows(share)

    def place(j, row):
        at = order_of_blocks.index(j)
        if row < first:
            return at * (first + SUB) + row
        return blocks * (first + SUB) + at * (share - first) + row - first

    signs = [parity_sign(jnp.bitwise_and(own, c), log2(blocks)) for c in range(chunks)]
    rows = 2 * SUB
    for start in range(0, side, rows):
        levels = [out[c * side + start : c * side + start + rows, :] for c in range(chunks)]
        if blocks == chunks:
            levels = [levels[0]] + [signs[c] * levels[c] for c in range(1, chunks)]
        for k in range(log2(chunks)):
            levels = butterfly(levels, 1 << k)
        for c in range(chunks):
            if blocks == chunks:
                messages[place(c, start) : place(c, start) + rows, :] = levels[c]
            else:
                out[c * side + start : c * side + start + rows, :] = levels[c]
    if blocks != chunks:
        for j in range(blocks):
            source = jnp.bitwise_xor(own, j) * share
            for low, size in ((0, first), (first, share - first)):
                rows_in = pl.ds(pl.multiple_of(source + low, SUB), size)
                messages[place(j, low) : place(j, low) + size, :] = out[rows_in, :]
    for k in range(blocks):
        at = k * (first + SUB) + first
        messages[at : at + SUB, :] = total


def transform_local(amplitudes, qubit_order, row_axis):
    parts, unmeasured, length = amplitudes.shape
    chunks = length // CHUNK
    side = ROW_SIDE * ROW_SIDE
    count = qubit_order.shape[0]
    return pl.pallas_call(
        functools.partial(transform_kernel, row_axis),
        out_shape=pltpu.VMEM((chunks * side + lax.axis_size(row_axis) * SUB, LANES), jnp.float32),
        in_specs=[pl.BlockSpec(memory_space=pl.ANY), pl.BlockSpec(memory_space=pl.ANY)],
        out_specs=pl.BlockSpec(memory_space=pltpu.VMEM),
        scratch_shapes=[
            pltpu.VMEM((parts, unmeasured, length), jnp.float32),
            pltpu.VMEM((chunks * side, LANES), jnp.float32),
            pltpu.VMEM((ROW_SIDE, ROW_SIDE, LANES), jnp.float32),
            pltpu.VMEM((2 * LANES, LANES), jnp.bfloat16),
            pltpu.VMEM((ROW_SIDE, LANES), jnp.float32),
            pltpu.SMEM((count,), jnp.int32),
            *[pltpu.SMEM((count + 1,), jnp.int32) for _ in range(6)],
            pltpu.SemaphoreType.DMA(()),
            pltpu.SemaphoreType.DMA((2 * chunks, parts)),
        ],
        name="transform_local",
    )(qubit_order, amplitudes)


def exchange(message, row_mask, col_mask):
    rows, cols = lax.axis_size("row"), lax.axis_size("col")
    mask = row_mask * cols + col_mask
    return lax.ppermute(message, ("row", "col"), [(i, i ^ mask) for i in range(rows * cols)])


def pick_of(bits, pick):
    return sum(1 << b for k, b in enumerate(bits) if pick >> k & 1)


def run_steps(blocks, steps, tail):
    for row_bits, col_bits in steps:
        dropped = pick_of(row_bits, -1)
        left = [j for j in blocks if j & dropped == 0]
        size = blocks[0].shape[0]
        signs = [1.0 - 2.0 * bit_of(lax.axis_index("col"), b).astype(jnp.float32) for b in col_bits]
        terms = []
        for row_pick in range(1 << len(row_bits)):
            row_mask = pick_of(row_bits, row_pick)
            joined = [blocks[j ^ row_mask] for j in left]
            message = joined[0] if len(joined) == 1 else jnp.concatenate(joined)
            for pick in range(1 << len(col_bits)):
                col_mask = pick_of(col_bits, pick)
                term = message
                if row_mask or col_mask:
                    term = exchange(message, row_mask, col_mask)
                terms.append((pick, term))
        blocks = {}
        for k, j in enumerate(left):
            values, summed = None, None
            for pick, term in terms:
                term = term[k * size : (k + 1) * size]
                part = term[: size - tail] if col_bits else term
                for n in range(len(col_bits)):
                    if not pick >> n & 1:
                        part = part * signs[n]
                values = part if values is None else values + part
                if tail and col_bits:
                    summed = term[size - tail :] if summed is None else summed + term[size - tail :]
            blocks[j] = jnp.concatenate([values, summed]) if tail and col_bits else values
    return blocks[0]


def local(amplitudes, qubit_order, measured_qubits):
    messages = transform_local(amplitudes, qubit_order, "row")
    count = lax.axis_size("row")
    row_bits, col_bits = log2(count), log2(lax.axis_size("col"))
    share = messages.shape[0] // count - SUB
    first = first_rows(share)
    first_blocks, second_blocks = {}, {}
    order_of_blocks = block_order(count)
    for at, j in enumerate(order_of_blocks):
        first_blocks[j] = messages[at * (first + SUB) : (at + 1) * (first + SUB)]
        start = count * (first + SUB) + at * (share - first)
        second_blocks[j] = messages[start : start + share - first]

    later = [((k,), ()) for k in range(2, row_bits)]
    first_steps = [((0,), ()), ((1,), (0,))] + later + [((), (b,)) for b in range(1, col_bits)]
    others = list(range(col_bits - 1))
    second_steps = [((0, 1), ())] + later + [((), (col_bits - 1,))]
    second_steps += [((), tuple(others[k : k + 2])) for k in range(0, len(others), 2)]
    one = run_steps(first_blocks, first_steps, SUB)
    two = run_steps(second_blocks, second_steps, 0)
    total = one[-SUB : 1 - SUB]
    values = jnp.concatenate([one[:-SUB], two])
    return (values * 2.0 ** (measured_qubits / 2) / total).reshape(1, -1)


def solution(mesh):
    def program(amplitudes, qubit_order):
        measured_qubits = log2(amplitudes.shape[2])

        def body(a, q):
            return local(a, q, measured_qubits)

        return jax.shard_map(
            body,
            mesh=mesh,
            in_specs=(P(None, "row", "col"), P()),
            out_specs=P("col", "row"),
            check_vma=False,
        )(amplitudes, qubit_order)

    return program
```
